256 devices in a mesh: dp: 32 (over y, z_hi, x), tensor: 8 (over z_lo, core).
Axes of the slice: x: 4, y: 4, z: 8 (z_hi: 2, z_lo: 4; z = z_hi * 4 + z_lo), core: 2. Of those that a mesh axis runs over, the one named last changes fastest.
Arguments:
- tokens: bfloat16 [1536, 6144], P('dp', 'tensor'), may hold values from -6 to 6
- out_grad: bfloat16 [1536, 6144], P('dp', 'tensor'), may hold values from -1.5 to 1.5
- expert_ids: int32 [1536, 2], P('dp'), may hold values from 0 to 3, all different within a row; in each aligned block of 48 rows (0 to 47, 48 to 95, ...) at most 32 rows name the same one
- gate_prob: bfloat16 [1536, 2], P('dp'), may hold values from 0.19921875 to 1
- gate_weight: bfloat16 [6144, 32768], P('tensor', 'dp'), may hold values from -0.078125 to 0.078125
- up_weight: bfloat16 [6144, 32768], P('tensor', 'dp'), may hold values from -0.078125 to 0.078125
- down_weight: bfloat16 [32768, 6144], P('dp', 'tensor'), may hold values from -0.0625 to 0.0625
Outputs:
- input_grad: bfloat16 [1536, 6144], P('dp', 'tensor')
- prob_grad: float32 [1536, 2], P('dp')
- gate_grad: bfloat16 [6144, 32768], P('tensor', 'dp')
- up_grad: bfloat16 [6144, 32768], P('tensor', 'dp')
- down_grad: bfloat16 [32768, 6144], P('dp', 'tensor')
The draws below stay inside these ranges and needn't reach their ends.
Inputs may be any that keep to these rules, and one draw needn't show every extreme that they name: `expert_ids`: the two ids of a token differ. Among the 48 tokens of one index of dp (aligned blocks of rows), no expert is named by more than 32 tokens, a bound that some block reaches.
All inputs are finite; a program needn't handle non-finite values.
Results may differ from the reference program's by a relative error of at most 0.0057.
Values may be sent and summed in bfloat16 or wider, within the bound.
A program may use at most 128 MiB of HBM per device.

```python
import math
import jax
import jax.numpy as jnp
import numpy as np

D = 6144
HID = 8192
EXPERTS = 4
TOK_DP = 48
CAP = 32
TOKENS = 1536
N_DP = 32


def block_levels(stream_key, dims, cuts, low, largest):
    def one(dim, shards_of):
        heights = jax.random.uniform(jax.random.fold_in(jax.random.fold_in(stream_key, 6), dim), (shards_of,), jnp.float32, low / len(cuts), largest / len(cuts))
        return jnp.repeat(jnp.exp(heights), dims[dim] // shards_of).reshape((-1,) + (1,) * (len(dims) - dim - 1))

    factor_of = one(*cuts[0])
    for cut in cuts[1:]:
        factor_of = factor_of * one(*cut)
    return factor_of


def shared_out(rng, own, number, rows, amount, top, reach, lean):
    ranking = jax.random.permutation(rng, amount)
    heavy_load, usual = load_shares(amount, rows * top, reach, lean, True), load_shares(amount, rows * top, reach, lean, False)
    places = jnp.arange(amount)

    def named(sizes, turn):
        used = int((sizes > 0).sum())
        fixed = max(1, used // 4)
        passed = fixed + (places - fixed + turn * (used - fixed)) % max(1, amount - fixed)
        return jnp.zeros((amount,), jnp.int32).at[ranking[jnp.where(places < fixed, places, passed)]].set(jnp.asarray(sizes, jnp.int32))

    sizes = jnp.where(number % 4 == 0, named(heavy_load, number // 4), named(usual, number - number // 4 - 1))
    mixed = jax.random.permutation(jax.random.fold_in(own, 3), amount)
    giver, sink = mixed[0:amount // 2 * 2:2], mixed[1:amount // 2 * 2:2]
    slack = jnp.minimum(sizes[giver] - 1, reach - sizes[sink]) // 2
    slack = jnp.where((giver == ranking[0]) | (sink == ranking[0]) | (sizes[sink] == 0), 0, jnp.maximum(slack, 0))
    passed = jax.random.randint(jax.random.fold_in(own, 4), (amount // 2,), 0, 1 << 20) % (slack + 1)
    sizes = sizes.at[giver].add(-passed).at[sink].add(passed)
    items = jnp.searchsorted(jnp.cumsum(sizes), jnp.arange(rows * top), side="right").astype(jnp.int32)
    listing = items.reshape(top, rows).T
    listing = listing[jax.random.permutation(jax.random.fold_in(own, 1), rows)]
    turn = jax.random.randint(jax.random.fold_in(own, 2), (rows, 1), 0, top)
    return jnp.take_along_axis(listing, (jnp.arange(top)[None, :] + turn) % top, axis=1)


def load_shares(count, total, limit, slope, full):
    weights = [(1 << 20) // math.isqrt(grade ** slope) + 1 for grade in range(1, count + 1)]
    largest = limit if full else min(limit, max(-(-total // count), total * weights[0] // sum(weights)))
    least = 1 if total - largest >= count - 1 else 0
    counts, rest = [largest] + [least] * (count - 1), total - largest - least * (count - 1)
    while rest > 0:
        free = [i for i in range(1, count) if counts[i] < largest] or [i for i in range(1, count) if counts[i] < limit]
        whole, budget = sum([weights[i] for i in free]), rest
        for i in free:
            addition = min(limit - counts[i], max(1, budget * weights[i] // whole), rest)
            counts[i] = counts[i] + addition
            rest = rest - addition
    return np.array(counts)


def normal_values(stream_key, extent, width, reach, cuts=(), kind=jnp.bfloat16):
    result = width * jax.random.normal(stream_key, extent, jnp.float32)
    if cuts:
        result = result * block_levels(stream_key, extent, cuts, -0.22, 0.18)
    return jnp.clip(result, -reach, reach).astype(kind)


def setup_inputs(seed: int = 0) -> dict:
    key_of = jax.random.split(jax.random.key(seed), 8)
    tokens = normal_values(key_of[0], (TOKENS, D), 1.0, 6.0, ((0, 32), (1, 8)))
    out_grad = normal_values(key_of[1], (TOKENS, D), 0.25, 1.5, ((0, 32), (1, 8)))
    expert_ids_keys = jax.random.split(jax.random.fold_in(key_of[2], 1), TOKENS // TOK_DP)
    expert_ids_turns = jax.random.permutation(jax.random.fold_in(key_of[2], 3), TOKENS // TOK_DP)
    expert_ids = jax.vmap(lambda own, number: shared_out(jax.random.fold_in(key_of[2], 2), own, number, TOK_DP, EXPERTS, 2, CAP, 2))(expert_ids_keys, expert_ids_turns).reshape((TOKENS, 2))
    gate_prob = jnp.clip(0.19921875 + 0.80078125 * jax.random.uniform(key_of[3], (TOKENS, 2), jnp.float32) ** block_levels(key_of[3], (TOKENS, 2), ((0, 32),), -0.2, 0.2), 0.19921875, 1.0).astype(jnp.bfloat16)
    gate_weight = normal_values(key_of[4], (D, EXPERTS * HID), D ** -0.5, 0.078125, ((0, 8), (1, 32)))
    up_weight = normal_values(key_of[5], (D, EXPERTS * HID), D ** -0.5, 0.078125, ((0, 8), (1, 32)))
    down_weight = normal_values(key_of[6], (EXPERTS * HID, D), HID ** -0.5, 0.0625, ((0, 32), (1, 8)))
    return {"tokens": tokens, "out_grad": out_grad, "expert_ids": expert_ids, "gate_prob": gate_prob, "gate_weight": gate_weight, "up_weight": up_weight, "down_weight": down_weight}


def slot_positions(expert_ids):
    labels = expert_ids.reshape(N_DP, 2 * TOK_DP).astype(jnp.int32)
    onehot = (labels[:, :, None] == jnp.arange(EXPERTS, dtype=jnp.int32)[None, None, :]).astype(jnp.int32)
    before = (jnp.cumsum(onehot, axis=1) - onehot).astype(jnp.int32)
    places = jnp.sum(before * onehot, axis=2).astype(jnp.int32)
    return labels, places


def reference(tokens, out_grad, expert_ids, gate_prob, gate_weight, up_weight, down_weight):
    labels, places = slot_positions(expert_ids)
    block_ids = jnp.arange(N_DP, dtype=jnp.int32)[:, None]
    slot_ids = (block_ids * (2 * TOK_DP) + jnp.arange(2 * TOK_DP, dtype=jnp.int32)[None, :]).reshape(-1).astype(jnp.int32)
    padded_tokens = jnp.concatenate([jnp.repeat(tokens, 2, axis=0), jnp.zeros((1, D), jnp.bfloat16)], axis=0)
    padded_grads = jnp.concatenate([jnp.repeat(out_grad, 2, axis=0), jnp.zeros((1, D), jnp.bfloat16)], axis=0)
    padded_probs = jnp.concatenate([gate_prob.reshape(-1).astype(jnp.float32), jnp.zeros((1,), jnp.float32)], axis=0)
    slot_grad = jnp.zeros((2 * TOKENS, D), jnp.float32)
    prob_slots = jnp.zeros((2 * TOKENS,), jnp.float32)
    gate_parts = []
    up_parts = []
    down_parts = []
    for expert in range(EXPERTS):
        target = jnp.where(labels == expert, block_ids * CAP + places, N_DP * CAP).reshape(-1).astype(jnp.int32)
        picked = jnp.full((N_DP * CAP,), 2 * TOKENS, jnp.int32).at[target].set(slot_ids, mode="drop")
        rows_in = padded_tokens[picked]
        grads_in = padded_grads[picked]
        probs_in = padded_probs[picked]
        gate_cols = gate_weight[:, expert * HID:(expert + 1) * HID]
        up_cols = up_weight[:, expert * HID:(expert + 1) * HID]
        down_rows = down_weight[expert * HID:(expert + 1) * HID, :]
        pre_gate = jnp.dot(rows_in, gate_cols, preferred_element_type=jnp.float32)
        pre_up = jnp.dot(rows_in, up_cols, preferred_element_type=jnp.float32)
        sigmoid_gate = jax.nn.sigmoid(pre_gate)
        hidden = (pre_gate * sigmoid_gate * pre_up).astype(jnp.bfloat16)
        back_hidden = jnp.dot(grads_in, down_rows.T, preferred_element_type=jnp.float32)
        prob_term = jnp.sum(hidden.astype(jnp.float32) * back_hidden, axis=1)
        hidden_grad = probs_in[:, None] * back_hidden
        gate_pre = (hidden_grad * pre_up * sigmoid_gate * (1.0 + pre_gate * (1.0 - sigmoid_gate))).astype(jnp.bfloat16)
        up_pre = (hidden_grad * pre_gate * sigmoid_gate).astype(jnp.bfloat16)
        scaled = (probs_in[:, None] * grads_in.astype(jnp.float32)).astype(jnp.bfloat16)
        input_part = jnp.dot(gate_pre, gate_cols.T, preferred_element_type=jnp.float32) + jnp.dot(up_pre, up_cols.T, preferred_element_type=jnp.float32)
        gate_parts.append(jnp.dot(rows_in.T, gate_pre, preferred_element_type=jnp.float32).astype(jnp.bfloat16))
        up_parts.append(jnp.dot(rows_in.T, up_pre, preferred_element_type=jnp.float32).astype(jnp.bfloat16))
        down_parts.append(jnp.dot(hidden.T, scaled, preferred_element_type=jnp.float32).astype(jnp.bfloat16))
        slot_grad = slot_grad.at[picked].add(input_part, mode="drop")
        prob_slots = prob_slots.at[picked].add(prob_term, mode="drop")
    input_grad = jnp.sum(slot_grad.reshape(TOKENS, 2, D), axis=1).astype(jnp.bfloat16)
    prob_grad = prob_slots.reshape(TOKENS, 2)
    gate_grad = jnp.concatenate(gate_parts, axis=1)
    up_grad = jnp.concatenate(up_parts, axis=1)
    down_grad = jnp.concatenate(down_parts, axis=0)
    return (input_grad, prob_grad, gate_grad, up_grad, down_grad)
```

```python
import functools

import jax
import jax.numpy as jnp
from jax import lax
from jax.experimental import pallas as pl
from jax.experimental.pallas import tpu as pltpu
from jax.sharding import PartitionSpec as P

EXPERTS = 4
CAP = 32
CHUNKS = 8
ROWS = EXPERTS * CAP
SUB = 32
PER = ROWS // SUB
NSUB = CHUNKS * PER
LAG = 2
QUARTER = 256
MESH = pl.DeviceIdType.MESH
F32 = jnp.float32
BF16 = jnp.bfloat16


def dot(a, b):
    return lax.dot_general(a, b, (((1,), (0,)), ((), ())), preferred_element_type=F32)


def dot_nt(a, b):
    return lax.dot_general(a, b, (((1,), (1,)), ((), ())), preferred_element_type=F32)


def dot_tn(a, b):
    return lax.dot_general(a, b, (((0,), (0,)), ((), ())), preferred_element_type=F32)


def kernel(
    width,
    x_ref,
    p_ref,
    wg_ref,
    wu_ref,
    wd_ref,
    out_x,
    out_p,
    out_g,
    out_u,
    out_d,
    x_other,
    p_other,
    rows,
    y_send,
    w_in,
    w_out,
    own,
    pair_send,
    pair_recv,
    line,
    hid,
    ret_send,
    ret_recv,
    pick,
    z_send,
    z_recv,
    acc_in,
    acc_out,
    turned,
    w_sem,
    z_s,
    z_r,
    y_s,
    y_r,
    x_s,
    x_r,
    pair_s,
    pair_r,
    line_s,
    line_r,
    cast_s,
    cast_r,
    core_s,
    core_r,
    ret_s,
    ret_r,
    last_s,
    last_r,
):
    dp = lax.axis_index("dp")
    tensor = lax.axis_index("tensor")
    y, zh, x = dp // 8, (dp // 4) % 2, dp % 4
    zl, core = tensor // 2, tensor % 2
    here = y * 4 + x
    lanes = 2 * width

    def at(y_, zh_, x_):
        return ((y_ * 2 + zh_) * 4 + x_, tensor)

    def plane(j):
        return at(j // 4, zh, j % 4)

    other_z = at(y, 1 - zh, x)
    partner = (dp, zl * 2 + 1 - core)
    above = (dp, (tensor + 2) % 8)
    below = (dp, (tensor + 6) % 8)

    def remote(src, dst, send, recv, device):
        return pltpu.make_async_remote_copy(
            src_ref=src, dst_ref=dst, send_sem=send, recv_sem=recv, device_id=device, device_id_type=MESH
        )

    w_copies = []
    for q in range(4):
        cols = pl.ds(q * QUARTER, QUARTER)
        w_copies.append(
            pltpu.make_async_copy(wg_ref.at[:, cols], w_in.at[q, :, pl.ds(0, QUARTER)], w_sem.at[2 * q])
        )
        w_copies.append(
            pltpu.make_async_copy(
                wu_ref.at[:, cols], w_in.at[q, :, pl.ds(QUARTER, QUARTER)], w_sem.at[2 * q + 1]
            )
        )
    w_copies.append(pltpu.make_async_copy(wd_ref, w_out, w_sem.at[8]))
    for copy in w_copies:
        copy.start()

    barrier = pltpu.get_barrier_semaphore()
    for o in range(1, 16):
        pl.semaphore_signal(barrier, inc=1, device_id=plane((here + o) % 16), device_id_type=MESH)
    pl.semaphore_signal(barrier, inc=1, device_id=other_z, device_id_type=MESH)
    pl.semaphore_signal(barrier, inc=1, device_id=partner, device_id_type=MESH)

    pl.semaphore_signal(barrier, inc=1, device_id=above, device_id_type=MESH)
    pl.semaphore_signal(barrier, inc=1, device_id=below, device_id_type=MESH)
    pl.semaphore_wait(barrier, 19)

    raw = [
        remote(x_ref, x_other, z_s.at[0], z_r.at[0], other_z),
        remote(p_ref, p_other, z_s.at[1], z_r.at[1], other_z),
    ]
    for copy in raw:
        copy.start()

    def y_copy(z, o):
        to = (y + o) % 4
        return remote(
            y_send.at[z, pl.ds(to * CAP, CAP)],
            rows.at[3 * z, pl.ds(y * CAP, CAP)],
            y_s.at[z, to],
            y_r.at[z, y],
            at(to, zh, x),
        )

    def y_wait(z, o):
        source = (y + o) % 4
        remote(
            y_send.at[z, pl.ds(source * CAP, CAP)],
            rows.at[3 * z, pl.ds(source * CAP, CAP)],
            y_s.at[z, source],
            y_r.at[z, source],
            at(source, zh, x),
        ).wait_recv()

    def choose(z, xs, ps):
        p = ps[...].astype(F32)
        one = jnp.where(p != 0.0, 1.0, 0.0).astype(BF16)
        prob = jnp.sum(jnp.abs(p), axis=1, keepdims=True)
        y_send[z, :, 0:lanes] = dot(one, xs[...]).astype(BF16)
        y_send[z, :, lanes : lanes + 128] = jnp.broadcast_to(prob, (ROWS, 128)).astype(BF16)
        for o in (1, 3, 2):
            y_copy(z, o).start()
        mine = pl.ds(pl.multiple_of(y * CAP, CAP), CAP)
        rows[3 * z, mine, :] = y_send[z, mine, :]

    right, left = at(y, zh, (x + 1) % 4), at(y, zh, (x + 3) % 4)
    half = ROWS // 2

    def x_copy(i):
        src, dst, lo, n, to = (
            (0, 1, 0, ROWS, right),
            (0, 2, 0, ROWS, left),
            (3, 4, 0, ROWS, right),
            (3, 5, 0, ROWS, left),
            (1, 7, 0, half, right),
            (2, 7, half, half, left),
            (4, 6, 0, half, right),
            (5, 6, half, half, left),
        )[i]
        part = pl.ds(lo, n)
        return remote(rows.at[src, part], rows.at[dst, part], x_s.at[i], x_r.at[i], to)

    def pair_copy(d, k):
        return remote(
            pair_send.at[k % 2, d],
            pair_recv.at[d, pl.ds(k * ROWS, ROWS)],
            pair_s.at[d, k],
            pair_r.at[d, k],
            partner,
        )

    def sub_rows(s):
        return pl.ds(pl.multiple_of(s * SUB, SUB), SUB)

    def line_copy(d, s):
        part = line.at[d, sub_rows(s)]
        return remote(part, part, line_s.at[d, s], line_r.at[d, s], below if d == 0 else above)

    def cast_copy(d, s):
        part = hid.at[2 * d + core, sub_rows(s)]
        return remote(part, part, cast_s.at[d, s], cast_r.at[d, s], above if d == 0 else below)

    def core_copy(d, s):
        part = hid.at[2 * d + core, sub_rows(s)]
        return remote(part, part, core_s.at[d, s], core_r.at[d, s], partner)

    def core_wait(d, s):
        part = hid.at[2 * d + 1 - core, sub_rows(s)]
        remote(part, part, core_s.at[d, s], core_r.at[d, s], partner).wait_recv()

    def project(k):
        @pl.when(k >= 2)
        def _():
            for d in range(2):
                pair_copy(d, k - 2).wait_send()

        for d in range(2):
            for mine in (False, True):
                q = 2 * d + (core if mine else 1 - core)
                up = dot(rows[k, :, 0:width], w_in[q])
                back = dot_nt(
                    rows[k, :, width:lanes],
                    w_out[pl.ds(pl.multiple_of(q * QUARTER, QUARTER), QUARTER), :],
                )
                if mine:
                    part = pl.ds(pl.multiple_of(k * ROWS, ROWS), ROWS)
                    own[d, part, 0 : 2 * QUARTER] = up
                    own[d, part, 2 * QUARTER : 3 * QUARTER] = back
                else:
                    pair_send[k % 2, d, :, 0 : 2 * QUARTER] = up
                    pair_send[k % 2, d, :, 2 * QUARTER : 3 * QUARTER] = back
                    pair_copy(d, k).start()

    def reduce(d, s):
        place = 3 - zl if d == 0 else zl

        @pl.when((s >= 0) & (s < NSUB))
        def _():
            @pl.when(s % PER == 0)
            def _():
                pair_copy(d, s // PER).wait_recv()

            part = sub_rows(s)

            @pl.when(place == 0)
            def _():
                line[d, part, :] = (own[d, part, :] + pair_recv[d, part, :]).astype(BF16)
                line_copy(d, s).start()

            @pl.when((place == 1) | (place == 2))
            def _():
                line_copy(d, s).wait_recv()
                total = own[d, part, :] + pair_recv[d, part, :] + line[d, part, :].astype(F32)
                line[d, part, :] = total.astype(BF16)
                line_copy(d, s).start()

            @pl.when(place == 3)
            def _():
                line_copy(d, s).wait_recv()
                total = own[d, part, :] + pair_recv[d, part, :] + line[d, part, :].astype(F32)
                gate = total[:, 0:QUARTER]
                up = total[:, QUARTER : 2 * QUARTER]
                back = total[:, 2 * QUARTER : 3 * QUARTER]
                inside = pl.ds(pl.multiple_of((s % PER) * SUB, SUB), SUB)
                prob = rows[s // PER, inside, lanes : lanes + 128].astype(F32)
                prob = jnp.concatenate([prob, prob], axis=1)
                sig = jax.nn.sigmoid(gate)
                hidden = (gate * sig * up).astype(BF16)
                grad = prob * back
                q = 2 * d + core
                hid[q, part, 0:QUARTER] = hidden
                hid[q, part, QUARTER : 2 * QUARTER] = (
                    grad * up * sig * (1.0 + gate * (1.0 - sig))
                ).astype(BF16)
                hid[q, part, 2 * QUARTER : 3 * QUARTER] = (grad * gate * sig).astype(BF16)
                term = jnp.sum(hidden.astype(F32) * back, axis=1, keepdims=True)
                hid[q, part, 3 * QUARTER : 3 * QUARTER + 128] = two_parts(term, SUB)
                cast_copy(d, s).start()
                core_copy(d, s).start()

    def two_parts(term, n):
        high = term.astype(BF16).astype(F32)
        lane = lax.broadcasted_iota(jnp.int32, (n, 128), 1)
        return jnp.where(lane < 64, high, term - high).astype(BF16)

    def spread(d, s):
        place = 3 - zl if d == 0 else zl

        @pl.when((s >= 0) & (s < NSUB) & (place < 3))
        def _():
            cast_copy(d, s).wait_recv()

            @pl.when(place > 0)
            def _():
                cast_copy(d, s).start()

            core_copy(d, s).start()

    def chunk_place(k):
        zi = jnp.where((k >= 3) & (k < 7), 1, 0)
        step = jnp.where(
            (k == 0) | (k == 3), 0, jnp.where((k == 1) | (k == 4), 3, jnp.where((k == 2) | (k == 5), 1, 2))
        )
        return zi, step

    def ret_copy(k, o):
        zi, step = chunk_place(k)
        to_y = (y + o) % 4
        return remote(
            ret_send.at[k % 2, pl.ds(to_y * CAP, CAP)],
            ret_recv.at[zi, here],
            ret_s.at[k, o],
            ret_r.at[zi, here],
            at(to_y, zh, (x + step) % 4),
        )

    def ret_wait(zi, o):
        source = (here + o) % 16
        remote(
            ret_send.at[0, pl.ds(0, CAP)],
            ret_recv.at[zi, source],
            ret_s.at[0, 0],
            ret_r.at[zi, source],
            plane(source),
        ).wait_recv()

    def ret_done(k):
        zi, step = chunk_place(k)

        @pl.when(step != 0)
        def _():
            ret_copy(k, 0).wait_send()

        for o in (1, 2, 3):
            ret_copy(k, o).wait_send()

    def back(k):
        for d in range(2):
            for i in range(PER):
                core_wait(d, k * PER + i)

        @pl.when(k >= 2)
        def _():
            ret_done(k - 2)

        part = pl.ds(pl.multiple_of(k * ROWS, ROWS), ROWS)
        total = dot_nt(hid[0, part, QUARTER : 3 * QUARTER], w_in[0])
        term = hid[0, part, 3 * QUARTER : 3 * QUARTER + 128].astype(F32)
        for q in range(1, 4):
            total += dot_nt(hid[q, part, QUARTER : 3 * QUARTER], w_in[q])
            term += hid[q, part, 3 * QUARTER : 3 * QUARTER + 128].astype(F32)
        ret_send[k % 2, :, 0:width] = total.astype(BF16)
        term = term[:, 0:1] + term[:, 64:65]
        ret_send[k % 2, :, width : width + 128] = two_parts(term, ROWS)
        zi, step = chunk_place(k)
        for o in (2, 1, 3):
            ret_copy(k, o).start()

        @pl.when(step != 0)
        def _():
            ret_copy(k, 0).start()

        @pl.when(step == 0)
        def _():
            mine = pl.ds(pl.multiple_of(y * CAP, CAP), CAP)
            ret_recv[zi, here] = ret_send[k % 2, mine, :]

    def weights(j):
        two = pl.ds(2 * j, 2)
        turned[...] = rows[two, :, 0:width].reshape(2 * ROWS, width).T
        prob = rows[two, :, lanes : lanes + 128].reshape(2 * ROWS, 128).astype(F32)
        grads = rows[two, :, width:lanes].reshape(2 * ROWS, width).astype(F32)
        scaled = (grads * jnp.concatenate([prob] * (width // 128), axis=1)).astype(BF16)
        part = pl.ds(pl.multiple_of(2 * j * ROWS, 2 * ROWS), 2 * ROWS)

        def one(q, _):
            acc_in[q] += dot(turned[...], hid[q, part, QUARTER : 3 * QUARTER])
            acc_out[q] += dot_tn(hid[q, part, 0:QUARTER], scaled)
            return 0

        lax.fori_loop(0, 4, one, 0)

    choose(0, x_ref, p_ref)
    acc_in[...] = jnp.zeros_like(acc_in)
    acc_out[...] = jnp.zeros_like(acc_out)
    for o in (1, 3, 2):
        y_wait(0, o)
    x_copy(0).start()
    x_copy(1).start()
    for copy in w_copies:
        copy.wait()
    project(0)

    up_end = 6 * LAG

    def tick(t, carry):
        for d in range(2):
            place = 3 - zl if d == 0 else zl
            spread(d, t - 3 * LAG - LAG * (3 - place))
        for d in range(2):
            place = 3 - zl if d == 0 else zl
            reduce(d, t - LAG * place)

        @pl.when(t == 1)
        def _():
            for copy in raw:
                copy.wait_recv()
            choose(1, x_other, p_other)

        @pl.when(((t + 1) % PER == 0) & (t + 1 < NSUB))
        def _():
            k = (t + 1) // PER

            @pl.when(k == 1)
            def _():
                x_copy(0).wait_recv()
                x_copy(4).start()
                for o in (1, 3, 2):
                    y_wait(1, o)
                x_copy(2).start()
                x_copy(3).start()

            @pl.when(k == 2)
            def _():
                x_copy(1).wait_recv()
                x_copy(5).start()

            @pl.when(k == 4)
            def _():
                x_copy(2).wait_recv()
                x_copy(6).start()

            @pl.when(k == 5)
            def _():
                x_copy(3).wait_recv()
                x_copy(7).start()

            @pl.when(k == 6)
            def _():
                x_copy(6).wait_recv()
                x_copy(7).wait_recv()

            @pl.when(k == 7)
            def _():
                x_copy(4).wait_recv()
                x_copy(5).wait_recv()

            project(k)

        @pl.when((t >= up_end + PER) & ((t - up_end) % PER == 0))
        def _():
            k = (t - up_end) // PER - 1
            back(k)

            @pl.when(k % 2 == 1)
            def _():
                weights(k // 2)

        return carry

    lax.fori_loop(0, NSUB + up_end + 1, tick, 0)

    for q in range(4):
        cols = pl.ds(q * QUARTER, QUARTER)
        out_g[:, cols] = acc_in[q, :, 0:QUARTER].astype(BF16)
        out_u[:, cols] = acc_in[q, :, QUARTER : 2 * QUARTER].astype(BF16)
        out_d[cols, :] = acc_out[q].astype(BF16)

    lane = lax.broadcasted_iota(jnp.int32, (x_ref.shape[0], 128), 1)

    def collect(zi, ps):
        for o in range(1, 16):
            ret_wait(zi, o)
        got = ret_recv[zi].reshape(16 * CAP, width + 128)
        p = ps[...].astype(F32)
        first = jnp.where(p > 0.0, 1.0, 0.0).astype(BF16)
        second = jnp.where(p < 0.0, 1.0, 0.0).astype(BF16)
        for i in range(16):
            part = pl.ds(i * CAP, CAP)
            e = (i // 4) * CAP
            pick[0, part, :] = first[e : e + CAP, :]
            pick[1, part, :] = second[e : e + CAP, :]
        both = pick[0] + pick[1]
        total = dot_tn(both, got[:, 0:width])
        terms = [dot_tn(pick[i], got[:, width : width + 128]) for i in range(2)]
        terms = [t[:, 0:1] + t[:, 64:65] for t in terms]
        highs = [t.astype(BF16).astype(F32) for t in terms]
        packed = jnp.where(
            lane < 64,
            jnp.where(lane < 32, highs[0], terms[0] - highs[0]),
            jnp.where(lane < 96, highs[1], terms[1] - highs[1]),
        )
        return total, packed

    total, packed = collect(1, p_other)
    z_send[:, 0:width] = total.astype(BF16)
    z_send[:, width : width + 128] = packed.astype(BF16)
    last = remote(z_send, z_recv, last_s.at[0], last_r.at[0], other_z)
    last.start()
    total, packed = collect(0, p_ref)
    last.wait_recv()
    out_x[...] = (total + z_recv[:, 0:width].astype(F32)).astype(BF16)
    out_p[...] = packed + z_recv[:, width : width + 128].astype(F32)

    last.wait_send()
    for copy in raw:
        copy.wait_send()
    for z in range(2):
        for o in (1, 2, 3):
            y_copy(z, o).wait_send()
    for i in range(8):
        x_copy(i).wait_send()
    for k in (CHUNKS - 2, CHUNKS - 1):
        for d in range(2):
            pair_copy(d, k).wait_send()
        ret_done(k)

    def drain(s, carry):
        for d in range(2):
            place = 3 - zl if d == 0 else zl

            @pl.when(place < 3)
            def _():
                line_copy(d, s).wait_send()

            @pl.when(place > 0)
            def _():
                cast_copy(d, s).wait_send()

            core_copy(d, s).wait_send()
        return carry

    lax.fori_loop(0, NSUB, drain, 0)


def layer(xs, ps, gate_weight, up_weight, down_weight):
    width, hid = gate_weight.shape
    tok = xs.shape[0]
    total = CHUNKS * ROWS
    vm = pltpu.VMEM
    dma = pltpu.SemaphoreType.DMA
    inner = pl.BlockSpec(memory_space=pltpu.VMEM)
    outer = pl.BlockSpec(memory_space=pl.ANY)
    message = 3 * QUARTER
    return pl.pallas_call(
        functools.partial(kernel, width),
        out_shape=(
            jax.ShapeDtypeStruct((tok, width), BF16),
            jax.ShapeDtypeStruct((tok, 128), F32),
            jax.ShapeDtypeStruct((width, hid), BF16),
            jax.ShapeDtypeStruct((width, hid), BF16),
            jax.ShapeDtypeStruct((hid, width), BF16),
        ),
        in_specs=[inner, inner, outer, outer, outer],
        out_specs=(inner,) * 5,
        scratch_shapes=[
            vm((tok, 2 * width), BF16),
            vm((ROWS, tok), BF16),
            vm((CHUNKS, ROWS, 2 * width + 128), BF16),
            vm((2, ROWS, 2 * width + 128), BF16),
            vm((4, width, 2 * QUARTER), BF16),
            vm((hid, width), BF16),
            vm((2, total, message), F32),
            vm((2, 2, ROWS, message), F32),
            vm((2, total, message), F32),
            vm((2, total, message), BF16),
            vm((4, total, message + 128), BF16),
            vm((2, ROWS, width + 128), BF16),
            vm((2, 16, CAP, width + 128), BF16),
            vm((2, 16 * CAP, tok), BF16),
            vm((tok, width + 128), BF16),
            vm((tok, width + 128), BF16),
            vm((4, width, 2 * QUARTER), F32),
            vm((4, QUARTER, width), F32),
            vm((width, 2 * ROWS), BF16),
            dma((9,)),
            dma((2,)),
            dma((2,)),
            dma((2, 4)),
            dma((2, 4)),
            dma((8,)),
            dma((8,)),
            dma((2, CHUNKS)),
            dma((2, CHUNKS)),
            dma((2, NSUB)),
            dma((2, NSUB)),
            dma((2, NSUB)),
            dma((2, NSUB)),
            dma((2, NSUB)),
            dma((2, NSUB)),
            dma((CHUNKS, 4)),
            dma((2, 16)),
            dma((1,)),
            dma((1,)),
        ],
        compiler_params=pltpu.CompilerParams(
            collective_id=0, has_side_effects=True, vmem_limit_bytes=67043328
        ),
    )(xs, ps, gate_weight, up_weight, down_weight)


def slot_probs(expert_ids, gate_prob):
    labels = expert_ids.reshape(-1)
    onehot = (labels[:, None] == jnp.arange(EXPERTS, dtype=jnp.int32)[None, :]).astype(jnp.int32)
    before = jnp.cumsum(onehot, axis=0) - onehot
    places = jnp.sum(before * onehot, axis=1)
    codes = (labels * CAP + places).reshape(-1, 2)
    slots = jnp.arange(ROWS, dtype=jnp.int32)[:, None]
    zero = jnp.zeros((), BF16)
    first = jnp.where(slots == codes[None, :, 0], gate_prob[None, :, 0], zero)
    second = jnp.where(slots == codes[None, :, 1], gate_prob[None, :, 1], zero)
    return first - second


def body(tokens, out_grad, expert_ids, gate_prob, gate_weight, up_weight, down_weight):
    xs = jnp.concatenate([tokens, out_grad], axis=1)
    ps = slot_probs(expert_ids, gate_prob)
    input_grad, terms, gate_grad, up_grad, down_grad = layer(xs, ps, gate_weight, up_weight, down_weight)
    prob_grad = jnp.stack([terms[:, 0] + terms[:, 32], terms[:, 64] + terms[:, 96]], axis=1)
    return (input_grad, prob_grad, gate_grad, up_grad, down_grad)


def solution(mesh):
    return jax.shard_map(
        body,
        mesh=mesh,
        in_specs=(
            P("dp", "tensor"),
            P("dp", "tensor"),
            P("dp", None),
            P("dp", None),
            P("tensor", "dp"),
            P("tensor", "dp"),
            P("dp", "tensor"),
        ),
        out_specs=(
            P("dp", "tensor"),
            P("dp", None),
            P("tensor", "dp"),
            P("tensor", "dp"),
            P("dp", "tensor"),
        ),
        check_vma=False,
    )
```

```python
import functools

import jax
import jax.numpy as jnp
from jax import lax
from jax.experimental import pallas as pl
from jax.experimental.pallas import tpu as pltpu
from jax.sharding import PartitionSpec as P

EXPERTS = 4
CAP = 32
CHUNKS = 8
ROWS = EXPERTS * CAP
SUB = 32
PER = ROWS // SUB
NSUB = CHUNKS * PER
LAG = 2
QUARTER = 256
MESH = pl.DeviceIdType.MESH
F32 = jnp.float32
BF16 = jnp.bfloat16


def dot(a, b):
    return lax.dot_general(a, b, (((1,), (0,)), ((), ())), preferred_element_type=F32)


def dot_nt(a, b):
    return lax.dot_general(a, b, (((1,), (1,)), ((), ())), preferred_element_type=F32)


def dot_tn(a, b):
    return lax.dot_general(a, b, (((0,), (0,)), ((), ())), preferred_element_type=F32)


def kernel(
    width,
    tok_ref,
    grad_ref,
    ids_ref,
    prob_ref,
    wg_ref,
    wu_ref,
    wd_ref,
    out_x,
    out_p,
    out_g,
    out_u,
    out_d,
    x_other,
    ids_other,
    prob_other,
    p_all,
    rows,
    y_send,
    w_in,
    w_out,
    own,
    pair_send,
    pair_recv,
    line,
    hid,
    ret_send,
    ret_recv,
    pick,
    z_send,
    z_recv,
    t_send,
    t_recv,
    acc_in,
    acc_out,
    turned,
    w_sem,
    z_s,
    z_r,
    y_s,
    y_r,
    x_s,
    x_r,
    pair_s,
    pair_r,
    line_s,
    line_r,
    cast_s,
    cast_r,
    core_s,
    core_r,
    ret_s,
    ret_r,
    last_s,
    last_r,
):
    dp = lax.axis_index("dp")
    tensor = lax.axis_index("tensor")
    y, zh, x = dp // 8, (dp // 4) % 2, dp % 4
    zl, core = tensor // 2, tensor % 2
    here = y * 4 + x
    lanes = 2 * width

    def at(y_, zh_, x_):
        return ((y_ * 2 + zh_) * 4 + x_, tensor)

    def plane(j):
        return at(j // 4, zh, j % 4)

    other_z = at(y, 1 - zh, x)
    partner = (dp, zl * 2 + 1 - core)
    above = (dp, (tensor + 2) % 8)
    below = (dp, (tensor + 6) % 8)

    def remote(src, dst, send, recv, device):
        return pltpu.make_async_remote_copy(
            src_ref=src, dst_ref=dst, send_sem=send, recv_sem=recv, device_id=device, device_id_type=MESH
        )

    w_copies = []
    for q in range(4):
        cols = pl.ds(q * QUARTER, QUARTER)
        w_copies.append(
            pltpu.make_async_copy(wg_ref.at[:, cols], w_in.at[q, :, pl.ds(0, QUARTER)], w_sem.at[2 * q])
        )
        w_copies.append(
            pltpu.make_async_copy(
                wu_ref.at[:, cols], w_in.at[q, :, pl.ds(QUARTER, QUARTER)], w_sem.at[2 * q + 1]
            )
        )
    w_copies.append(pltpu.make_async_copy(wd_ref, w_out, w_sem.at[8]))
    for copy in w_copies:
        copy.start()

    barrier = pltpu.get_barrier_semaphore()
    for o in range(1, 16):
        pl.semaphore_signal(barrier, inc=1, device_id=plane((here + o) % 16), device_id_type=MESH)
    pl.semaphore_signal(barrier, inc=1, device_id=other_z, device_id_type=MESH)
    pl.semaphore_signal(barrier, inc=1, device_id=partner, device_id_type=MESH)

    pl.semaphore_signal(barrier, inc=1, device_id=above, device_id_type=MESH)
    pl.semaphore_signal(barrier, inc=1, device_id=below, device_id_type=MESH)
    raw = [
        remote(ids_ref, ids_other, z_s.at[0], z_r.at[0], other_z),
        remote(prob_ref, prob_other, z_s.at[1], z_r.at[1], other_z),
        remote(tok_ref, x_other.at[0], z_s.at[2], z_r.at[2], other_z),
        remote(grad_ref, x_other.at[1], z_s.at[3], z_r.at[3], other_z),
    ]

    def y_copy(z, o):
        to = (y + o) % 4
        return remote(
            y_send.at[z, pl.ds(to * CAP, CAP)],
            rows.at[3 * z, pl.ds(y * CAP, CAP)],
            y_s.at[z, to],
            y_r.at[z, y],
            at(to, zh, x),
        )

    def y_wait(z, o):
        source = (y + o) % 4
        remote(
            y_send.at[z, pl.ds(source * CAP, CAP)],
            rows.at[3 * z, pl.ds(source * CAP, CAP)],
            y_s.at[z, source],
            y_r.at[z, source],
            at(source, zh, x),
        ).wait_recv()

    def choose(z, toks, grads, ids, probs):
        count = ids.shape[1]
        named = lax.broadcasted_iota(jnp.int32, (8, count), 0)
        member = jnp.where((named == ids[0:1, :]) | (named == ids[1:2, :]), 1.0, 0.0)
        earlier = jnp.where(
            lax.broadcasted_iota(jnp.int32, (count, count), 0)
            < lax.broadcasted_iota(jnp.int32, (count, count), 1),
            1.0,
            0.0,
        )
        before = dot(member.astype(BF16), earlier.astype(BF16))
        slot = lax.broadcasted_iota(jnp.int32, (CAP, count), 0).astype(F32)
        for e in range(EXPERTS):
            value = jnp.where(ids[0:1, :] == e, probs[0:1, :], -probs[1:2, :])
            value = jnp.where(member[e : e + 1, :] > 0.0, value, 0.0)
            p_all[z, e * CAP : (e + 1) * CAP, :] = jnp.where(slot == before[e : e + 1, :], value, 0.0)
        p = p_all[z]
        one = jnp.where(p != 0.0, 1.0, 0.0).astype(BF16)
        prob = jnp.sum(jnp.abs(p), axis=1, keepdims=True)
        y_send[z, :, 0:width] = dot(one, toks).astype(BF16)
        y_send[z, :, width:lanes] = dot(one, grads).astype(BF16)
        y_send[z, :, lanes : lanes + 128] = jnp.broadcast_to(prob, (ROWS, 128)).astype(BF16)

    def deal(z):
        for o in (1, 3, 2):
            y_copy(z, o).start()
        mine = pl.ds(pl.multiple_of(y * CAP, CAP), CAP)
        rows[3 * z, mine, :] = y_send[z, mine, :]

    right, left = at(y, zh, (x + 1) % 4), at(y, zh, (x + 3) % 4)
    half = ROWS // 2

    def x_copy(i):
        src, dst, lo, n, to = (
            (0, 1, 0, ROWS, right),
            (0, 2, 0, ROWS, left),
            (3, 4, 0, ROWS, right),
            (3, 5, 0, ROWS, left),
            (1, 7, 0, half, right),
            (2, 7, half, half, left),
            (4, 6, 0, half, right),
            (5, 6, half, half, left),
        )[i]
        part = pl.ds(lo, n)
        return remote(rows.at[src, part], rows.at[dst, part], x_s.at[i], x_r.at[i], to)

    def pair_copy(d, k):
        return remote(
            pair_send.at[k % 2, d],
            pair_recv.at[d, pl.ds(k * ROWS, ROWS)],
            pair_s.at[d, k],
            pair_r.at[d, k],
            partner,
        )

    def sub_rows(s):
        return pl.ds(pl.multiple_of(s * SUB, SUB), SUB)

    def line_copy(d, s):
        part = line.at[d, sub_rows(s)]
        return remote(part, part, line_s.at[d, s], line_r.at[d, s], below if d == 0 else above)

    def cast_copy(d, s):
        part = hid.at[2 * d + core, sub_rows(s)]
        return remote(part, part, cast_s.at[d, s], cast_r.at[d, s], above if d == 0 else below)

    def core_copy(d, s):
        part = hid.at[2 * d + core, sub_rows(s)]
        return remote(part, part, core_s.at[d, s], core_r.at[d, s], partner)

    def core_wait(d, s):
        part = hid.at[2 * d + 1 - core, sub_rows(s)]
        remote(part, part, core_s.at[d, s], core_r.at[d, s], partner).wait_recv()

    def project(k):
        @pl.when(k >= 2)
        def _():
            for d in range(2):
                pair_copy(d, k - 2).wait_send()

        for d in range(2):
            for mine in (False, True):
                q = 2 * d + (core if mine else 1 - core)
                up = dot(rows[k, :, 0:width], w_in[q])
                back = dot_nt(
                    rows[k, :, width:lanes],
                    w_out[pl.ds(pl.multiple_of(q * QUARTER, QUARTER), QUARTER), :],
                )
                if mine:
                    part = pl.ds(pl.multiple_of(k * ROWS, ROWS), ROWS)
                    own[d, part, 0 : 2 * QUARTER] = up
                    own[d, part, 2 * QUARTER : 3 * QUARTER] = back
                else:
                    pair_send[k % 2, d, :, 0 : 2 * QUARTER] = up
                    pair_send[k % 2, d, :, 2 * QUARTER : 3 * QUARTER] = back
                    pair_copy(d, k).start()

    def reduce(d, s):
        place = 3 - zl if d == 0 else zl

        @pl.when((s >= 0) & (s < NSUB))
        def _():
            @pl.when(s % PER == 0)
            def _():
                pair_copy(d, s // PER).wait_recv()

            part = sub_rows(s)

            @pl.when(place == 0)
            def _():
                line[d, part, :] = (own[d, part, :] + pair_recv[d, part, :]).astype(BF16)
                line_copy(d, s).start()

            @pl.when((place == 1) | (place == 2))
            def _():
                line_copy(d, s).wait_recv()
                total = own[d, part, :] + pair_recv[d, part, :] + line[d, part, :].astype(F32)
                line[d, part, :] = total.astype(BF16)
                line_copy(d, s).start()

            @pl.when(place == 3)
            def _():
                line_copy(d, s).wait_recv()
                total = own[d, part, :] + pair_recv[d, part, :] + line[d, part, :].astype(F32)
                gate = total[:, 0:QUARTER]
                up = total[:, QUARTER : 2 * QUARTER]
                back = total[:, 2 * QUARTER : 3 * QUARTER]
                inside = pl.ds(pl.multiple_of((s % PER) * SUB, SUB), SUB)
                prob = rows[s // PER, inside, lanes : lanes + 128].astype(F32)
                prob = jnp.concatenate([prob, prob], axis=1)
                sig = jax.nn.sigmoid(gate)
                hidden = (gate * sig * up).astype(BF16)
                grad = prob * back
                q = 2 * d + core
                hid[q, part, 0:QUARTER] = hidden
                hid[q, part, QUARTER : 2 * QUARTER] = (
                    grad * up * sig * (1.0 + gate * (1.0 - sig))
                ).astype(BF16)
                hid[q, part, 2 * QUARTER : 3 * QUARTER] = (grad * gate * sig).astype(BF16)
                term = jnp.sum(hidden.astype(F32) * back, axis=1, keepdims=True)
                hid[q, part, 3 * QUARTER : 3 * QUARTER + 128] = two_parts(term, SUB)
                cast_copy(d, s).start()
                core_copy(d, s).start()

    def two_parts(term, n):
        high = term.astype(BF16).astype(F32)
        lane = lax.broadcasted_iota(jnp.int32, (n, 128), 1)
        return jnp.where(lane < 64, high, term - high).astype(BF16)

    def spread(d, s):
        place = 3 - zl if d == 0 else zl

        @pl.when((s >= 0) & (s < NSUB) & (place < 3))
        def _():
            cast_copy(d, s).wait_recv()

            @pl.when(place > 0)
            def _():
                cast_copy(d, s).start()

            core_copy(d, s).start()

    def chunk_place(k):
        zi = jnp.where((k >= 3) & (k < 7), 1, 0)
        step = jnp.where(
            (k == 0) | (k == 3), 0, jnp.where((k == 1) | (k == 4), 3, jnp.where((k == 2) | (k == 5), 1, 2))
        )
        return zi, step

    def ret_copy(k, o):
        zi, step = chunk_place(k)
        to_y = (y + o) % 4
        return remote(
            ret_send.at[k % 2, pl.ds(to_y * CAP, CAP)],
            ret_recv.at[zi, here],
            ret_s.at[k, o],
            ret_r.at[zi, here],
            at(to_y, zh, (x + step) % 4),
        )

    def ret_wait(zi, o):
        source = (here + o) % 16
        remote(
            ret_send.at[0, pl.ds(0, CAP)],
            ret_recv.at[zi, source],
            ret_s.at[0, 0],
            ret_r.at[zi, source],
            plane(source),
        ).wait_recv()

    def ret_done(k):
        zi, step = chunk_place(k)

        @pl.when(step != 0)
        def _():
            ret_copy(k, 0).wait_send()

        for o in (1, 2, 3):
            ret_copy(k, o).wait_send()

    def back(k):
        for d in range(2):
            for i in range(PER):
                core_wait(d, k * PER + i)

        @pl.when(k >= 2)
        def _():
            ret_done(k - 2)

        part = pl.ds(pl.multiple_of(k * ROWS, ROWS), ROWS)
        total = dot_nt(hid[0, part, QUARTER : 3 * QUARTER], w_in[0])
        term = hid[0, part, 3 * QUARTER : 3 * QUARTER + 128].astype(F32)
        for q in range(1, 4):
            total += dot_nt(hid[q, part, QUARTER : 3 * QUARTER], w_in[q])
            term += hid[q, part, 3 * QUARTER : 3 * QUARTER + 128].astype(F32)
        ret_send[k % 2, :, 0:width] = total.astype(BF16)
        term = term[:, 0:1] + term[:, 64:65]
        ret_send[k % 2, :, width : width + 128] = two_parts(term, ROWS)
        zi, step = chunk_place(k)
        for o in (2, 1, 3):
            ret_copy(k, o).start()

        @pl.when(step != 0)
        def _():
            ret_copy(k, 0).start()

        @pl.when(step == 0)
        def _():
            mine = pl.ds(pl.multiple_of(y * CAP, CAP), CAP)
            ret_recv[zi, here] = ret_send[k % 2, mine, :]

    def weights(j):
        two = pl.ds(2 * j, 2)
        turned[...] = rows[two, :, 0:width].reshape(2 * ROWS, width).T
        prob = rows[two, :, lanes : lanes + 128].reshape(2 * ROWS, 128).astype(F32)
        grads = rows[two, :, width:lanes].reshape(2 * ROWS, width).astype(F32)
        scaled = (grads * jnp.concatenate([prob] * (width // 128), axis=1)).astype(BF16)
        part = pl.ds(pl.multiple_of(2 * j * ROWS, 2 * ROWS), 2 * ROWS)

        def one(q, _):
            up = dot(turned[...], hid[q, part, QUARTER : 3 * QUARTER])
            down = dot_tn(hid[q, part, 0:QUARTER], scaled)

            @pl.when(j == 0)
            def _():
                acc_in[q] = up
                acc_out[q] = down

            @pl.when((j > 0) & (j < CHUNKS // 2 - 1))
            def _():
                acc_in[q] += up
                acc_out[q] += down

            @pl.when(j == CHUNKS // 2 - 1)
            def _():
                cols = pl.ds(pl.multiple_of(q * QUARTER, QUARTER), QUARTER)
                out_g[:, cols] = (acc_in[q, :, 0:QUARTER] + up[:, 0:QUARTER]).astype(BF16)
                out_u[:, cols] = (acc_in[q, :, QUARTER : 2 * QUARTER] + up[:, QUARTER : 2 * QUARTER]).astype(BF16)
                out_d[cols, :] = (acc_out[q] + down).astype(BF16)

            return 0

        lax.fori_loop(0, 4, one, 0)

    choose(0, tok_ref[...], grad_ref[...], ids_ref[...], prob_ref[...].astype(F32))
    pl.semaphore_wait(barrier, 19)
    deal(0)
    for copy in raw:
        copy.start()
    for o in (1, 3, 2):
        y_wait(0, o)
    x_copy(0).start()
    x_copy(1).start()
    for copy in w_copies:
        copy.wait()
    project(0)

    def collect(zi):
        for o in range(1, 16):
            ret_wait(zi, o)
        got = ret_recv[zi].reshape(16 * CAP, width + 128)
        p = p_all[zi]
        first = jnp.where(p > 0.0, 1.0, 0.0).astype(BF16)
        second = jnp.where(p < 0.0, 1.0, 0.0).astype(BF16)
        for i in range(16):
            part = pl.ds(i * CAP, CAP)
            e = (i // 4) * CAP
            pick[0, part, :] = first[e : e + CAP, :]
            pick[1, part, :] = second[e : e + CAP, :]
        terms = [dot_tn(got[:, width : width + 128], pick[i]) for i in range(2)]
        terms = [t[0:1, :] + t[64:65, :] for t in terms]
        return dot_tn(pick[0] + pick[1], got[:, 0:width]), jnp.concatenate(terms, axis=0)

    last = [
        remote(z_send, z_recv, last_s.at[0], last_r.at[0], other_z),
        remote(t_send, t_recv, last_s.at[1], last_r.at[1], other_z),
    ]

    up_end = 6 * LAG

    def tick(t, carry):
        for d in range(2):
            place = 3 - zl if d == 0 else zl
            spread(d, t - 3 * LAG - LAG * (3 - place))
        for d in range(2):
            place = 3 - zl if d == 0 else zl
            reduce(d, t - LAG * place)

        @pl.when(t == 1)
        def _():
            for copy in raw:
                copy.wait_recv()
            choose(1, x_other[0], x_other[1], ids_other[...], prob_other[...].astype(F32))
            deal(1)

        @pl.when(((t + 1) % PER == 0) & (t + 1 < NSUB))
        def _():
            k = (t + 1) // PER

            @pl.when(k == 1)
            def _():
                x_copy(0).wait_recv()
                x_copy(4).start()
                for o in (1, 3, 2):
                    y_wait(1, o)
                x_copy(2).start()
                x_copy(3).start()

            @pl.when(k == 2)
            def _():
                x_copy(1).wait_recv()
                x_copy(5).start()

            @pl.when(k == 4)
            def _():
                x_copy(2).wait_recv()
                x_copy(6).start()

            @pl.when(k == 5)
            def _():
                x_copy(3).wait_recv()
                x_copy(7).start()

            @pl.when(k == 6)
            def _():
                x_copy(6).wait_recv()
                x_copy(7).wait_recv()

            @pl.when(k == 7)
            def _():
                x_copy(4).wait_recv()
                x_copy(5).wait_recv()

            project(k)

        @pl.when((t >= up_end + PER) & ((t - up_end) % PER == 0))
        def _():
            k = (t - up_end) // PER - 1
            back(k)

            @pl.when(k == CHUNKS - 1)
            def _():
                grads, terms = collect(1)
                z_send[...] = grads.astype(BF16)
                t_send[...] = terms
                for copy in last:
                    copy.start()

            @pl.when(k % 2 == 1)
            def _():
                weights(k // 2)

        return carry

    lax.fori_loop(0, NSUB + up_end + 1, tick, 0)

    grads, terms = collect(0)
    for copy in last:
        copy.wait_recv()
    out_x[...] = (grads + z_recv[...].astype(F32)).astype(BF16)
    out_p[...] = terms + t_recv[...]

    for copy in last:
        copy.wait_send()
    for copy in raw:
        copy.wait_send()
    for z in range(2):
        for o in (1, 2, 3):
            y_copy(z, o).wait_send()
    for i in range(8):
        x_copy(i).wait_send()
    for k in (CHUNKS - 2, CHUNKS - 1):
        for d in range(2):
            pair_copy(d, k).wait_send()
        ret_done(k)

    def drain(s, carry):
        for d in range(2):
            place = 3 - zl if d == 0 else zl

            @pl.when(place < 3)
            def _():
                line_copy(d, s).wait_send()

            @pl.when(place > 0)
            def _():
                cast_copy(d, s).wait_send()

            core_copy(d, s).wait_send()
        return carry

    lax.fori_loop(0, NSUB, drain, 0)


def layer(tokens, out_grad, ids, probs, gate_weight, up_weight, down_weight):
    width, hid = gate_weight.shape
    tok = tokens.shape[0]
    total = CHUNKS * ROWS
    vm = pltpu.VMEM
    dma = pltpu.SemaphoreType.DMA
    inner = pl.BlockSpec(memory_space=pltpu.VMEM)
    outer = pl.BlockSpec(memory_space=pl.ANY)
    message = 3 * QUARTER
    return pl.pallas_call(
        functools.partial(kernel, width),
        out_shape=(
            vm((tok, width), BF16),
            vm((2, tok), F32),
            vm((width, hid), BF16),
            vm((width, hid), BF16),
            vm((hid, width), BF16),
        ),
        in_specs=[inner, inner, inner, inner, outer, outer, outer],
        out_specs=(inner,) * 5,
        scratch_shapes=[
            vm((2, tok, width), BF16),
            vm((2, tok), jnp.int32),
            vm((2, tok), BF16),
            vm((2, ROWS, tok), F32),
            vm((CHUNKS, ROWS, 2 * width + 128), BF16),
            vm((2, ROWS, 2 * width + 128), BF16),
            vm((4, width, 2 * QUARTER), BF16),
            vm((hid, width), BF16),
            vm((2, total, message), F32),
            vm((2, 2, ROWS, message), F32),
            vm((2, total, message), F32),
            vm((2, total, message), BF16),
            vm((4, total, message + 128), BF16),
            vm((2, ROWS, width + 128), BF16),
            vm((2, 16, CAP, width + 128), BF16),
            vm((2, 16 * CAP, tok), BF16),
            vm((tok, width), BF16),
            vm((tok, width), BF16),
            vm((2, tok), F32),
            vm((2, tok), F32),
            vm((4, width, 2 * QUARTER), F32),
            vm((4, QUARTER, width), F32),
            vm((width, 2 * ROWS), BF16),
            dma((9,)),
            dma((4,)),
            dma((4,)),
            dma((2, 4)),
            dma((2, 4)),
            dma((8,)),
            dma((8,)),
            dma((2, CHUNKS)),
            dma((2, CHUNKS)),
            dma((2, NSUB)),
            dma((2, NSUB)),
            dma((2, NSUB)),
            dma((2, NSUB)),
            dma((2, NSUB)),
            dma((2, NSUB)),
            dma((CHUNKS, 4)),
            dma((2, 16)),
            dma((2,)),
            dma((2,)),
        ],
        compiler_params=pltpu.CompilerParams(
            collective_id=0, has_side_effects=True, vmem_limit_bytes=55 * 1024 * 1024
        ),
    )(tokens, out_grad, ids, probs, gate_weight, up_weight, down_weight)


def body(tokens, out_grad, expert_ids, gate_prob, gate_weight, up_weight, down_weight):
    input_grad, terms, gate_grad, up_grad, down_grad = layer(
        tokens, out_grad, expert_ids.T, gate_prob.T, gate_weight, up_weight, down_weight
    )
    return (input_grad, terms.T, gate_grad, up_grad, down_grad)


def solution(mesh):
    return jax.shard_map(
        body,
        mesh=mesh,
        in_specs=(
            P("dp", "tensor"),
            P("dp", "tensor"),
            P("dp", None),
            P("dp", None),
            P("tensor", "dp"),
            P("tensor", "dp"),
            P("dp", "tensor"),
        ),
        out_specs=(
            P("dp", "tensor"),
            P("dp", None),
            P("tensor", "dp"),
            P("tensor", "dp"),
            P("dp", "tensor"),
        ),
        check_vma=False,
    )
```

```python
import functools

import jax
import jax.numpy as jnp
from jax import lax
from jax.experimental import pallas as pl
from jax.experimental.pallas import tpu as pltpu
from jax.sharding import PartitionSpec as P

EXPERTS = 4
CAP = 32
CHUNKS = 8
ROWS = EXPERTS * CAP
SUB = 32
PER = ROWS // SUB
NSUB = CHUNKS * PER
LAG = 2
QUARTER = 256
MESH = pl.DeviceIdType.MESH
F32 = jnp.float32
BF16 = jnp.bfloat16


def dot(a, b):
    return lax.dot_general(a, b, (((1,), (0,)), ((), ())), preferred_element_type=F32)


def dot_nt(a, b):
    return lax.dot_general(a, b, (((1,), (1,)), ((), ())), preferred_element_type=F32)


def dot_tn(a, b):
    return lax.dot_general(a, b, (((0,), (0,)), ((), ())), preferred_element_type=F32)


def kernel(
    width,
    tok_ref,
    grad_ref,
    ids_ref,
    prob_ref,
    wg_ref,
    wu_ref,
    wd_ref,
    out_x,
    out_p,
    out_g,
    out_u,
    out_d,
    x_other,
    ids_other,
    prob_other,
    p_all,
    rows,
    y_send,
    w_in,
    w_out,
    own,
    pair_send,
    pair_recv,
    line,
    hid,
    ret_send,
    ret_recv,
    pick,
    z_send,
    z_recv,
    t_send,
    t_recv,
    acc_in,
    acc_out,
    turned,
    scaled,
    term_send,
    term_recv,
    term_all,
    w_sem,
    z_s,
    z_r,
    y_s,
    y_r,
    x_s,
    x_r,
    far_s,
    far_r,
    pair_s,
    pair_r,
    line_s,
    line_r,
    cast_s,
    cast_r,
    core_s,
    core_r,
    ret_s,
    ret_r,
    last_s,
    last_r,
    term_s,
    term_r,
    all_s,
    all_r,
):
    dp = lax.axis_index("dp")
    tensor = lax.axis_index("tensor")
    y, zh, x = dp // 8, (dp // 4) % 2, dp % 4
    zl, core = tensor // 2, tensor % 2
    here = y * 4 + x
    lanes = 2 * width

    def at(y_, zh_, x_):
        return ((y_ * 2 + zh_) * 4 + x_, tensor)

    def plane(j):
        return at(j // 4, zh, j % 4)

    other_z = at(y, 1 - zh, x)
    partner = (dp, zl * 2 + 1 - core)
    root = (zl == 0) | (zl == 3)
    above = (dp, (tensor + 2) % 8)
    below = (dp, (tensor + 6) % 8)

    def remote(src, dst, send, recv, device):
        return pltpu.make_async_remote_copy(
            src_ref=src, dst_ref=dst, send_sem=send, recv_sem=recv, device_id=device, device_id_type=MESH
        )

    w_copies = []
    for q in range(4):
        cols = pl.ds(q * QUARTER, QUARTER)
        w_copies.append(
            pltpu.make_async_copy(wg_ref.at[:, cols], w_in.at[q, :, pl.ds(0, QUARTER)], w_sem.at[2 * q])
        )
        w_copies.append(
            pltpu.make_async_copy(
                wu_ref.at[:, cols], w_in.at[q, :, pl.ds(QUARTER, QUARTER)], w_sem.at[2 * q + 1]
            )
        )
    w_copies.append(pltpu.make_async_copy(wd_ref, w_out, w_sem.at[8]))
    for copy in w_copies:
        copy.start()

    barrier = pltpu.get_barrier_semaphore()
    for o in range(1, 16):
        pl.semaphore_signal(barrier, inc=1, device_id=plane((here + o) % 16), device_id_type=MESH)
    pl.semaphore_signal(barrier, inc=1, device_id=other_z, device_id_type=MESH)
    for o in range(1, 8):
        pl.semaphore_signal(barrier, inc=1, device_id=(dp, (tensor + o) % 8), device_id_type=MESH)

    raw = [
        remote(ids_ref, ids_other, z_s.at[0], z_r.at[0], other_z),
        remote(prob_ref, prob_other, z_s.at[1], z_r.at[1], other_z),
        remote(tok_ref, x_other.at[0], z_s.at[2], z_r.at[2], other_z),
        remote(grad_ref, x_other.at[1], z_s.at[3], z_r.at[3], other_z),
    ]

    def offset(g):
        return jnp.where(g == 2, 3, jnp.where(g == 3, 2, g))

    def group(g):
        return pl.ds(g * CAP, CAP)

    def y_copy(z, o):
        to = (y + o) % 4
        g = (None, 2, 3, 1)[o]
        return remote(
            y_send.at[z, pl.ds(to * CAP, CAP)],
            rows.at[2 * z, group(g)],
            y_s.at[z, o],
            y_r.at[z, g],
            at(to, zh, x),
        )

    def y_wait(z, g):
        part = rows.at[2 * z, group(g)]
        remote(part, part, y_s.at[z, 0], y_r.at[z, g], other_z).wait_recv()

    def choose(z, toks, grads, ids, probs):
        count = ids.shape[1]
        named = lax.broadcasted_iota(jnp.int32, (8, count), 0)
        member = jnp.where((named == ids[0:1, :]) | (named == ids[1:2, :]), 1.0, 0.0)
        earlier = jnp.where(
            lax.broadcasted_iota(jnp.int32, (count, count), 0)
            < lax.broadcasted_iota(jnp.int32, (count, count), 1),
            1.0,
            0.0,
        )
        before = dot(member.astype(BF16), earlier.astype(BF16))
        slot = lax.broadcasted_iota(jnp.int32, (CAP, count), 0).astype(F32)
        for e in range(EXPERTS):
            value = jnp.where(ids[0:1, :] == e, probs[0:1, :], -probs[1:2, :])
            value = jnp.where(member[e : e + 1, :] > 0.0, value, 0.0)
            p_all[z, e * CAP : (e + 1) * CAP, :] = jnp.where(slot == before[e : e + 1, :], value, 0.0)
        p = p_all[z]
        one = jnp.where(p != 0.0, 1.0, 0.0).astype(BF16)
        prob = jnp.sum(jnp.abs(p), axis=1, keepdims=True)
        y_send[z, :, 0:width] = dot(one, toks).astype(BF16)
        y_send[z, :, width:lanes] = dot(one, grads).astype(BF16)
        y_send[z, :, lanes : lanes + 128] = jnp.broadcast_to(prob, (ROWS, 128)).astype(BF16)

    def deal(z):
        for o in (1, 3, 2):
            y_copy(z, o).start()
        rows[2 * z, 0:CAP, :] = y_send[z, pl.ds(pl.multiple_of(y * CAP, CAP), CAP), :]
        for side in range(2):
            x_copy(z, side, 0).start()

    right, left = at(y, zh, (x + 1) % 4), at(y, zh, (x + 3) % 4)
    half = ROWS // 2

    def x_copy(z, side, g):
        dst = ((1, 7), (3, 4))[z][side]
        return remote(
            rows.at[2 * z, group(g)],
            rows.at[dst, group(g)],
            x_s.at[z, side, g],
            x_r.at[z, side, g],
            (right, left)[side],
        )

    def x_pass(z):
        for g in (1, 2, 3):
            y_wait(z, g)
            for side in range(2):
                x_copy(z, side, g).start()

    def x_wait(z):
        for side in range(2):
            for g in range(4):
                x_copy(z, side, g).wait_recv()

    def far_copy(i):
        src, dst, lo, to = (
            (1, 6, 0, right),
            (7, 6, half, left),
            (3, 5, 0, right),
            (4, 5, half, left),
        )[i]
        part = pl.ds(lo, half)
        return remote(rows.at[src, part], rows.at[dst, part], far_s.at[i], far_r.at[i], to)

    def pair_copy(d, k):
        return remote(
            pair_send.at[k % 2, d],
            pair_recv.at[d, pl.ds(k * ROWS, ROWS)],
            pair_s.at[d, k],
            pair_r.at[d, k],
            partner,
        )

    def sub_rows(s):
        return pl.ds(pl.multiple_of(s * SUB, SUB), SUB)

    def line_copy(d, s):
        part = line.at[d, sub_rows(s)]
        return remote(part, part, line_s.at[d, s], line_r.at[d, s], below if d == 0 else above)

    def cast_copy(d, s):
        part = hid.at[2 * d + core, sub_rows(s)]
        return remote(part, part, cast_s.at[d, s], cast_r.at[d, s], above if d == 0 else below)

    def core_copy(d, s):
        part = hid.at[2 * d + core, sub_rows(s)]
        return remote(part, part, core_s.at[d, s], core_r.at[d, s], partner)

    def core_wait(d, s):
        part = hid.at[2 * d + 1 - core, sub_rows(s)]
        remote(part, part, core_s.at[d, s], core_r.at[d, s], partner).wait_recv()

    def project(k):
        @pl.when(k >= 2)
        def _():
            for d in range(2):
                pair_copy(d, k - 2).wait_send()

        for d in range(2):
            for mine in (False, True):
                q = 2 * d + (core if mine else 1 - core)
                up = dot(rows[k, :, 0:width], w_in[q])
                back = dot_nt(
                    rows[k, :, width:lanes],
                    w_out[pl.ds(pl.multiple_of(q * QUARTER, QUARTER), QUARTER), :],
                )
                if mine:
                    part = pl.ds(pl.multiple_of(k * ROWS, ROWS), ROWS)
                    own[d, part, 0 : 2 * QUARTER] = up
                    own[d, part, 2 * QUARTER : 3 * QUARTER] = back
                else:
                    pair_send[k % 2, d, :, 0 : 2 * QUARTER] = up
                    pair_send[k % 2, d, :, 2 * QUARTER : 3 * QUARTER] = back
                    pair_copy(d, k).start()

    def reduce(d, s):
        place = 3 - zl if d == 0 else zl

        @pl.when((s >= 0) & (s < NSUB))
        def _():
            @pl.when(s % PER == 0)
            def _():
                pair_copy(d, s // PER).wait_recv()

            part = sub_rows(s)

            @pl.when(place == 0)
            def _():
                line[d, part, :] = (own[d, part, :] + pair_recv[d, part, :]).astype(BF16)
                line_copy(d, s).start()

            @pl.when((place == 1) | (place == 2))
            def _():
                line_copy(d, s).wait_recv()
                total = own[d, part, :] + pair_recv[d, part, :] + line[d, part, :].astype(F32)
                line[d, part, :] = total.astype(BF16)
                line_copy(d, s).start()

            @pl.when(place == 3)
            def _():
                line_copy(d, s).wait_recv()
                total = own[d, part, :] + pair_recv[d, part, :] + line[d, part, :].astype(F32)
                gate = total[:, 0:QUARTER]
                up = total[:, QUARTER : 2 * QUARTER]
                back = total[:, 2 * QUARTER : 3 * QUARTER]
                inside = pl.ds(pl.multiple_of((s % PER) * SUB, SUB), SUB)
                prob = rows[s // PER, inside, lanes : lanes + 128].astype(F32)
                prob = jnp.concatenate([prob, prob], axis=1)
                sig = jax.nn.sigmoid(gate)
                hidden = (gate * sig * up).astype(BF16)
                grad = prob * back
                q = 2 * d + core
                hid[q, part, 0:QUARTER] = hidden
                hid[q, part, QUARTER : 2 * QUARTER] = (
                    grad * up * sig * (1.0 + gate * (1.0 - sig))
                ).astype(BF16)
                hid[q, part, 2 * QUARTER : 3 * QUARTER] = (grad * gate * sig).astype(BF16)
                term = jnp.sum(hidden.astype(F32) * back, axis=1, keepdims=True)
                cast_copy(d, s).start()
                core_copy(d, s).start()
                term_send[s] = two_parts(term, SUB)
                zi, step = chunk_place(s // PER)
                self_too = (s % PER == 0) & (step == 0)

                @pl.when(self_too)
                def _():
                    term_recv[zi, here] = term_send[s]

                @pl.when(jnp.logical_not(self_too))
                def _():
                    term_copy(s).start()

    def term_copy(s):
        zi, step = chunk_place(s // PER)
        to_y = (y + offset(s % PER)) % 4
        return remote(
            term_send.at[s],
            term_recv.at[zi, here],
            term_s.at[s],
            term_r.at[zi, here],
            at(to_y, zh, (x + step) % 4),
        )

    def two_parts(term, n):
        high = term.astype(BF16).astype(F32)
        lane = lax.broadcasted_iota(jnp.int32, (n, 128), 1)
        return jnp.where(lane < 64, high, term - high).astype(BF16)

    def spread(d, s):
        place = 3 - zl if d == 0 else zl

        @pl.when((s >= 0) & (s < NSUB) & (place < 3))
        def _():
            cast_copy(d, s).wait_recv()

            @pl.when(place > 0)
            def _():
                cast_copy(d, s).start()

            core_copy(d, s).start()

    def chunk_place(k):
        zi = jnp.where((k >= 2) & (k < 6), 1, 0)
        step = jnp.where(
            (k == 0) | (k == 2), 0, jnp.where((k == 1) | (k == 3), 3, jnp.where((k == 4) | (k == 7), 1, 2))
        )
        return zi, step

    def ret_copy(k, g):
        zi, step = chunk_place(k)
        to_y = (y + (0, 1, 3, 2)[g]) % 4
        return remote(
            ret_send.at[k % 2, group(g)],
            ret_recv.at[zi, here],
            ret_s.at[k, g],
            ret_r.at[zi, here],
            at(to_y, zh, (x + step) % 4),
        )

    def ret_wait(zi, o):
        source = (here + o) % 16
        remote(
            ret_send.at[0, pl.ds(0, CAP)],
            ret_recv.at[zi, source],
            ret_s.at[0, 0],
            ret_r.at[zi, source],
            plane(source),
        ).wait_recv()

    def ret_done(k):
        zi, step = chunk_place(k)

        @pl.when(step != 0)
        def _():
            ret_copy(k, 0).wait_send()

        for o in (1, 2, 3):
            ret_copy(k, o).wait_send()

    def back(k):
        for d in range(2):
            for i in range(PER):
                core_wait(d, k * PER + i)

        @pl.when(k >= 2)
        def _():
            ret_done(k - 2)

        part = pl.ds(pl.multiple_of(k * ROWS, ROWS), ROWS)
        total = dot_nt(hid[0, part, QUARTER : 3 * QUARTER], w_in[0])
        for q in range(1, 4):
            total += dot_nt(hid[q, part, QUARTER : 3 * QUARTER], w_in[q])
        ret_send[k % 2] = total.astype(BF16)
        zi, step = chunk_place(k)
        for g in (3, 1, 2):
            ret_copy(k, g).start()

        @pl.when(step != 0)
        def _():
            ret_copy(k, 0).start()

        @pl.when(step == 0)
        def _():
            ret_recv[zi, here] = ret_send[k % 2, 0:CAP, :]

    def weights_in(j):
        two = pl.ds(2 * j, 2)
        turned[...] = rows[two, :, 0:width].reshape(2 * ROWS, width).T
        prob = rows[two, :, lanes : lanes + 128].reshape(2 * ROWS, 128).astype(F32)
        grads = rows[two, :, width:lanes].reshape(2 * ROWS, width).astype(F32)
        scaled[...] = (grads * jnp.concatenate([prob] * (width // 128), axis=1)).astype(BF16)

    def weights(j, q):
        part = pl.ds(pl.multiple_of(2 * j * ROWS, 2 * ROWS), 2 * ROWS)
        up = dot(turned[...], hid[q, part, QUARTER : 3 * QUARTER])
        down = dot_tn(hid[q, part, 0:QUARTER], scaled[...])

        @pl.when(j == 0)
        def _():
            acc_in[q] = up
            acc_out[q] = down

        @pl.when((j > 0) & (j < CHUNKS // 2 - 1))
        def _():
            acc_in[q] += up
            acc_out[q] += down

        @pl.when(j == CHUNKS // 2 - 1)
        def _():
            cols = pl.ds(pl.multiple_of(q * QUARTER, QUARTER), QUARTER)
            out_g[:, cols] = (acc_in[q, :, 0:QUARTER] + up[:, 0:QUARTER]).astype(BF16)
            out_u[:, cols] = (acc_in[q, :, QUARTER : 2 * QUARTER] + up[:, QUARTER : 2 * QUARTER]).astype(BF16)
            out_d[cols, :] = (acc_out[q] + down).astype(BF16)

    choose(0, tok_ref[...], grad_ref[...], ids_ref[...], prob_ref[...].astype(F32))
    pl.semaphore_wait(barrier, 23)
    deal(0)
    for copy in raw:
        copy.start()
    x_pass(0)
    for copy in w_copies:
        copy.wait()
    project(0)

    def chosen(zi):
        p = p_all[zi]
        first = jnp.where(p > 0.0, 1.0, 0.0).astype(BF16)
        second = jnp.where(p < 0.0, 1.0, 0.0).astype(BF16)
        for i in range(16):
            part = pl.ds(i * CAP, CAP)
            e = (i // 4) * CAP
            pick[0, part, :] = first[e : e + CAP, :]
            pick[1, part, :] = second[e : e + CAP, :]

    def collect(zi):
        for o in range(1, 16):
            ret_wait(zi, o)
        chosen(zi)
        return dot_tn(pick[0] + pick[1], ret_recv[zi].reshape(16 * CAP, width))

    def collect_terms(zi):
        for o in range(1, 16):
            source = (here + o) % 16
            part = term_recv.at[zi, source]
            remote(part, part, term_s.at[0], term_r.at[zi, source], plane(source)).wait_recv()
        chosen(zi)
        got = term_recv[zi].reshape(16 * CAP, 128)
        terms = [dot_tn(got, pick[i]) for i in range(2)]
        terms = [t[0:1, :] + t[64:65, :] for t in terms]
        return jnp.concatenate(terms, axis=0)

    slot = jnp.where(zl == 3, 2, 0) + core

    def all_copy(o):
        return remote(
            term_all.at[slot],
            term_all.at[slot],
            all_s.at[o],
            all_r.at[slot],
            (dp, (tensor + o) % 8),
        )

    last = remote(z_send, z_recv, last_s.at[0], last_r.at[0], other_z)
    last_term = remote(t_send, t_recv, last_s.at[1], last_r.at[1], other_z)

    up_end = 6 * LAG

    def tick(t, carry):
        for d in range(2):
            place = 3 - zl if d == 0 else zl
            spread(d, t - 3 * LAG - LAG * (3 - place))
        for d in range(2):
            place = 3 - zl if d == 0 else zl
            reduce(d, t - LAG * place)

        @pl.when(t == 1)
        def _():
            for copy in raw:
                copy.wait_recv()
            choose(1, x_other[0], x_other[1], ids_other[...], prob_other[...].astype(F32))
            deal(1)

        @pl.when(t == PER + 1)
        def _():
            x_pass(1)

        @pl.when(((t + 1) % PER == 0) & (t + 1 < NSUB))
        def _():
            k = (t + 1) // PER

            @pl.when(k == 1)
            def _():
                x_wait(0)
                far_copy(0).start()
                far_copy(1).start()

            @pl.when(k == 3)
            def _():
                x_wait(1)
                far_copy(2).start()
                far_copy(3).start()

            @pl.when(k == 5)
            def _():
                far_copy(2).wait_recv()
                far_copy(3).wait_recv()

            @pl.when(k == 6)
            def _():
                far_copy(0).wait_recv()
                far_copy(1).wait_recv()

            project(k)

        u = t - up_end

        @pl.when((u >= PER) & (u % PER == 0))
        def _():
            back(u // PER - 1)

        v = u - 2 * PER
        j, m = v // (2 * PER), v % (2 * PER)

        @pl.when((v > 0) & ((m == 1) | (m == 2) | (m == 5) | (m == 6)))
        def _():
            q = jnp.where(m < 3, m - 1, m - 3)

            @pl.when(q == 0)
            def _():
                weights_in(j)

            weights(j, q)

        @pl.when(u == 6 * PER + PER - 1)
        def _():
            z_send[...] = collect(1).astype(BF16)
            last.start()

            @pl.when(root)
            def _():
                t_send[...] = collect_terms(1)
                last_term.start()

        @pl.when((u == 8 * PER - 1) & root)
        def _():
            terms = collect_terms(0)
            last_term.wait_recv()
            term_all[slot] = terms + t_recv[...]
            for o in range(1, 8):
                all_copy(o).start()

        return carry

    lax.fori_loop(0, NSUB + up_end + 1, tick, 0)

    weights_in(CHUNKS // 2 - 1)

    def ending(q, carry):
        weights(CHUNKS // 2 - 1, q)
        return carry

    lax.fori_loop(0, 4, ending, 0)
    grads = collect(0)
    last.wait_recv()
    out_x[...] = (grads + z_recv[...].astype(F32)).astype(BF16)
    for i in range(4):
        source = (0, 1, 6, 7)[i]

        @pl.when(tensor != source)
        def _():
            part = term_all.at[i]
            remote(part, part, all_s.at[0], all_r.at[i], partner).wait_recv()

    out_p[...] = term_all[0] + term_all[1] + term_all[2] + term_all[3]
    last.wait_send()

    @pl.when(root)
    def _():
        last_term.wait_send()
        for o in range(1, 8):
            all_copy(o).wait_send()

        def drain_terms(s, carry):
            zi, step = chunk_place(s // PER)

            @pl.when(jnp.logical_not((s % PER == 0) & (step == 0)))
            def _():
                term_copy(s).wait_send()

            return carry

        lax.fori_loop(0, NSUB, drain_terms, 0)

    for copy in raw:
        copy.wait_send()
    for z in range(2):
        for o in (1, 2, 3):
            y_copy(z, o).wait_send()
        for side in range(2):
            for g in range(4):
                x_copy(z, side, g).wait_send()
    for i in range(4):
        far_copy(i).wait_send()
    for k in (CHUNKS - 2, CHUNKS - 1):
        for d in range(2):
            pair_copy(d, k).wait_send()
        ret_done(k)

    def drain(s, carry):
        for d in range(2):
            place = 3 - zl if d == 0 else zl

            @pl.when(place < 3)
            def _():
                line_copy(d, s).wait_send()

            @pl.when(place > 0)
            def _():
                cast_copy(d, s).wait_send()

            core_copy(d, s).wait_send()
        return carry

    lax.fori_loop(0, NSUB, drain, 0)


def layer(tokens, out_grad, ids, probs, gate_weight, up_weight, down_weight):
    width, hid = gate_weight.shape
    tok = tokens.shape[0]
    total = CHUNKS * ROWS
    vm = pltpu.VMEM
    dma = pltpu.SemaphoreType.DMA
    inner = pl.BlockSpec(memory_space=pltpu.VMEM)
    outer = pl.BlockSpec(memory_space=pl.ANY)
    message = 3 * QUARTER
    return pl.pallas_call(
        functools.partial(kernel, width),
        out_shape=(
            vm((tok, width), BF16),
            vm((2, tok), F32),
            vm((width, hid), BF16),
            vm((width, hid), BF16),
            vm((hid, width), BF16),
        ),
        in_specs=[inner, inner, inner, inner, outer, outer, outer],
        out_specs=(inner,) * 5,
        scratch_shapes=[
            vm((2, tok, width), BF16),
            vm((2, tok), jnp.int32),
            vm((2, tok), BF16),
            vm((2, ROWS, tok), F32),
            vm((CHUNKS, ROWS, 2 * width + 128), BF16),
            vm((2, ROWS, 2 * width + 128), BF16),
            vm((4, width, 2 * QUARTER), BF16),
            vm((hid, width), BF16),
            vm((2, total, message), F32),
            vm((2, 2, ROWS, message), F32),
            vm((2, total, message), F32),
            vm((2, total, message), BF16),
            vm((4, total, message), BF16),
            vm((2, ROWS, width), BF16),
            vm((2, 16, CAP, width), BF16),
            vm((2, 16 * CAP, tok), BF16),
            vm((tok, width), BF16),
            vm((tok, width), BF16),
            vm((2, tok), F32),
            vm((2, tok), F32),
            vm((4, width, 2 * QUARTER), F32),
            vm((4, QUARTER, width), F32),
            vm((width, 2 * ROWS), BF16),
            vm((2 * ROWS, width), BF16),
            vm((NSUB, CAP, 128), BF16),
            vm((2, 16, CAP, 128), BF16),
            vm((4, 2, tok), F32),
            dma((9,)),
            dma((4,)),
            dma((4,)),
            dma((2, 4)),
            dma((2, 4)),
            dma((2, 2, 4)),
            dma((2, 2, 4)),
            dma((4,)),
            dma((4,)),
            dma((2, CHUNKS)),
            dma((2, CHUNKS)),
            dma((2, NSUB)),
            dma((2, NSUB)),
            dma((2, NSUB)),
            dma((2, NSUB)),
            dma((2, NSUB)),
            dma((2, NSUB)),
            dma((CHUNKS, 4)),
            dma((2, 16)),
            dma((2,)),
            dma((2,)),
            dma((NSUB,)),
            dma((2, 16)),
            dma((8,)),
            dma((4,)),
        ],
        compiler_params=pltpu.CompilerParams(
            collective_id=0, has_side_effects=True, vmem_limit_bytes=55 * 1024 * 1024
        ),
    )(tokens, out_grad, ids, probs, gate_weight, up_weight, down_weight)


def body(tokens, out_grad, expert_ids, gate_prob, gate_weight, up_weight, down_weight):
    input_grad, terms, gate_grad, up_grad, down_grad = layer(
        tokens, out_grad, expert_ids.T, gate_prob.T, gate_weight, up_weight, down_weight
    )
    return (input_grad, terms.T, gate_grad, up_grad, down_grad)


def solution(mesh):
    return jax.shard_map(
        body,
        mesh=mesh,
        in_specs=(
            P("dp", "tensor"),
            P("dp", "tensor"),
            P("dp", None),
            P("dp", None),
            P("tensor", "dp"),
            P("tensor", "dp"),
            P("dp", "tensor"),
        ),
        out_specs=(
            P("dp", "tensor"),
            P("dp", None),
            P("tensor", "dp"),
            P("tensor", "dp"),
            P("dp", "tensor"),
        ),
        check_vma=False,
    )
```

```python
import functools

import jax
import jax.numpy as jnp
from jax import lax
from jax.experimental import pallas as pl
from jax.experimental.pallas import tpu as pltpu
from jax.sharding import PartitionSpec as P

EXPERTS = 4
CAP = 32
CHUNKS = 8
ROWS = EXPERTS * CAP
SUB = 32
PER = ROWS // SUB
PARTS = ((0, CAP, 0), (CAP, 2 * CAP, CHUNKS), (3 * CAP, CAP, CHUNKS + 1))
NSUB = CHUNKS * PER
LAG = 2
QUARTER = 256
TERMS_1 = 23
TERMS_0 = 29
TURN = 31
MESH = pl.DeviceIdType.MESH
F32 = jnp.float32
BF16 = jnp.bfloat16


def dot(a, b):
    return lax.dot_general(a, b, (((1,), (0,)), ((), ())), preferred_element_type=F32)


def dot_nt(a, b):
    return lax.dot_general(a, b, (((1,), (1,)), ((), ())), preferred_element_type=F32)


def dot_tn(a, b):
    return lax.dot_general(a, b, (((0,), (0,)), ((), ())), preferred_element_type=F32)


def kernel(
    width,
    tok_ref,
    grad_ref,
    ids_ref,
    prob_ref,
    wg_ref,
    wu_ref,
    wd_ref,
    out_x,
    out_p,
    out_g,
    out_u,
    out_d,
    x_other,
    ids_other,
    prob_other,
    p_all,
    rows,
    y_send,
    w_in,
    w_out,
    own,
    pair_send,
    pair_recv,
    line,
    hid,
    ret_send,
    ret_recv,
    pick,
    z_send,
    z_recv,
    t_send,
    t_recv,
    acc_in,
    acc_out,
    turned,
    scaled,
    term_send,
    term_recv,
    term_all,
    w_sem,
    z_s,
    z_r,
    y_s,
    y_r,
    x_s,
    x_r,
    far_s,
    far_r,
    pair_s,
    pair_r,
    line_s,
    line_r,
    cast_s,
    cast_r,
    core_s,
    core_r,
    ret_s,
    ret_r,
    last_s,
    last_r,
    term_s,
    term_r,
    all_s,
    all_r,
):
    dp = lax.axis_index("dp")
    tensor = lax.axis_index("tensor")
    y, zh, x = dp // 8, (dp // 4) % 2, dp % 4
    zl, core = tensor // 2, tensor % 2
    here = y * 4 + x
    lanes = 2 * width

    def at(y_, zh_, x_):
        return ((y_ * 2 + zh_) * 4 + x_, tensor)

    def plane(j):
        return at(j // 4, zh, j % 4)

    other_z = at(y, 1 - zh, x)
    partner = (dp, zl * 2 + 1 - core)
    root = (zl == 0) | (zl == 3)
    above = (dp, (tensor + 2) % 8)
    below = (dp, (tensor + 6) % 8)

    def remote(src, dst, send, recv, device):
        return pltpu.make_async_remote_copy(
            src_ref=src, dst_ref=dst, send_sem=send, recv_sem=recv, device_id=device, device_id_type=MESH
        )

    for q in range(4):
        cols = pl.ds(q * QUARTER, QUARTER)
        for i, ref in ((0, wg_ref), (1, wu_ref)):
            pltpu.make_async_copy(
                ref.at[:, cols], w_in.at[q, :, pl.ds(i * QUARTER, QUARTER)], w_sem.at[0]
            ).start()
    pltpu.make_async_copy(wd_ref, w_out, w_sem.at[1]).start()

    barrier = pltpu.get_barrier_semaphore()
    for o in range(1, 16):
        pl.semaphore_signal(barrier, inc=1, device_id=plane((here + o) % 16), device_id_type=MESH)
    pl.semaphore_signal(barrier, inc=1, device_id=other_z, device_id_type=MESH)
    for o in range(1, 8):
        pl.semaphore_signal(barrier, inc=1, device_id=(dp, (tensor + o) % 8), device_id_type=MESH)

    raw = [
        remote(ids_ref, ids_other, z_s.at[0], z_r.at[0], other_z),
        remote(prob_ref, prob_other, z_s.at[1], z_r.at[1], other_z),
        remote(tok_ref, x_other.at[0], z_s.at[2], z_r.at[2], other_z),
        remote(grad_ref, x_other.at[1], z_s.at[3], z_r.at[3], other_z),
    ]

    def offset(g):
        return jnp.where(g == 2, 3, jnp.where(g == 3, 2, g))

    def group(g):
        return pl.ds(g * CAP, CAP)

    def y_copy(z, o):
        to = (y + o) % 4
        g = (None, 2, 3, 1)[o]
        return remote(
            y_send.at[z, pl.ds(to * CAP, CAP)],
            rows.at[3 * z, group(g)],
            y_s.at[z],
            y_r.at[z, g],
            at(to, zh, x),
        )

    def y_wait(z, g):
        part = rows.at[3 * z, group(g)]
        remote(part, part, y_s.at[z], y_r.at[z, g], other_z).wait_recv()

    def choose(z, toks, grads, ids, probs):
        count = ids.shape[1]
        named = lax.broadcasted_iota(jnp.int32, (8, count), 0)
        member = jnp.where((named == ids[0:1, :]) | (named == ids[1:2, :]), 1.0, 0.0)
        earlier = jnp.where(
            lax.broadcasted_iota(jnp.int32, (count, count), 0)
            < lax.broadcasted_iota(jnp.int32, (count, count), 1),
            1.0,
            0.0,
        )
        before = dot(member.astype(BF16), earlier.astype(BF16))
        slot = lax.broadcasted_iota(jnp.int32, (CAP, count), 0).astype(F32)
        for e in range(EXPERTS):
            value = jnp.where(ids[0:1, :] == e, probs[0:1, :], -probs[1:2, :])
            value = jnp.where(member[e : e + 1, :] > 0.0, value, 0.0)
            p_all[z, e * CAP : (e + 1) * CAP, :] = jnp.where(slot == before[e : e + 1, :], value, 0.0)
        p = p_all[z]
        one = jnp.where(p != 0.0, 1.0, 0.0).astype(BF16)
        prob = jnp.sum(jnp.abs(p), axis=1, keepdims=True)
        y_send[z, :, 0:width] = dot(one, toks).astype(BF16)
        y_send[z, :, width:lanes] = dot(one, grads).astype(BF16)
        y_send[z, :, lanes : lanes + 128] = jnp.broadcast_to(prob, (ROWS, 128)).astype(BF16)

    def place_own(z):
        rows[3 * z, 0:CAP, :] = y_send[z, pl.ds(pl.multiple_of(y * CAP, CAP), CAP), :]

    def deal(z):
        for o in (1, 3, 2):
            y_copy(z, o).start()
        for side in range(2):
            x_copy(z, side, 0).start()

    right, left = at(y, zh, (x + 1) % 4), at(y, zh, (x + 3) % 4)
    half = ROWS // 2

    def x_copy(z, side, g):
        dst = ((1, 2), (4, 6))[z][g // 2]
        return remote(
            rows.at[3 * z, group(g)],
            rows.at[dst, group(2 * side + g % 2)],
            x_s.at[z],
            x_r.at[z, g // 2],
            (right, left)[side],
        )

    def x_pass(z, gs):
        for g in gs:
            y_wait(z, g)
            for side in range(2):
                x_copy(z, side, g).start()

    def x_wait(z, h):
        part = rows.at[0]
        remote(part, part, x_s.at[z], x_r.at[z, h], other_z).wait_recv()

    def far_copy(i):
        src, dst, lo, to = (
            (1, 7, 0, right),
            (2, 7, half, left),
            (4, 5, 0, right),
            (6, 5, half, left),
        )[i]
        part = pl.ds(lo, half)
        return remote(rows.at[src, part], rows.at[dst, part], far_s.at[0], far_r.at[i // 2], to)

    def far_wait(h):
        part = rows.at[0]
        remote(part, part, far_s.at[0], far_r.at[h], other_z).wait_recv()

    def pair_copy(d, k, lo=0, n=ROWS, i=None):
        i = k if i is None else i
        return remote(
            pair_send.at[k, d, pl.ds(lo, n)],
            pair_recv.at[d, pl.ds(k * ROWS + lo, n)],
            pair_s.at[d],
            pair_r.at[d, i],
            partner,
        )

    def sub_rows(s):
        return pl.ds(pl.multiple_of(s * SUB, SUB), SUB)

    def line_copy(d, s):
        part = line.at[d, sub_rows(s)]
        return remote(part, part, line_s.at[d], line_r.at[d, s], below if d == 0 else above)

    def cast_copy(d, s):
        part = hid.at[2 * d + core, sub_rows(s)]
        return remote(part, part, cast_s.at[d], cast_r.at[d, s], above if d == 0 else below)

    def core_copy(d, s):
        part = hid.at[2 * d + core, sub_rows(s)]
        return remote(part, part, core_s.at[d], core_r.at[d, s // (PER // 2)], partner)

    def core_wait(d, h):
        part = hid.at[2 * d + 1 - core, pl.ds(pl.multiple_of(h * ROWS // 2, ROWS // 2), ROWS // 2)]
        remote(part, part, core_s.at[d], core_r.at[d, h], partner).wait_recv()

    def project(k, lo=0, n=ROWS, i=None):
        take = pl.ds(lo, n)
        for d in range(2):
            for mine in (False, True):
                q = 2 * d + (core if mine else 1 - core)
                up = dot(rows[k, take, 0:width], w_in[q])
                back = dot_nt(
                    rows[k, take, width:lanes],
                    w_out[pl.ds(pl.multiple_of(q * QUARTER, QUARTER), QUARTER), :],
                )
                if mine:
                    part = pl.ds(pl.multiple_of(k * ROWS + lo, CAP), n)
                    own[d, part, 0 : 2 * QUARTER] = up
                    own[d, part, 2 * QUARTER : 3 * QUARTER] = back
                else:
                    pair_send[k, d, take, 0 : 2 * QUARTER] = up
                    pair_send[k, d, take, 2 * QUARTER : 3 * QUARTER] = back
                    if i != 0:
                        pair_copy(d, k, lo, n, i).start()

    def reduce(d, s):
        place = 3 - zl if d == 0 else zl

        @pl.when((s >= 0) & (s < NSUB))
        def _():
            @pl.when((s % PER == 0) & (s > 0))
            def _():
                pair_copy(d, s // PER).wait_recv()

            for lo, n, i in PARTS:

                @pl.when(s == lo // SUB)
                def _():
                    pair_copy(d, 0, lo, n, i).wait_recv()

            part = sub_rows(s)

            @pl.when(place == 0)
            def _():
                line[d, part, :] = (own[d, part, :] + pair_recv[d, part, :]).astype(BF16)
                line_copy(d, s).start()

            @pl.when((place == 1) | (place == 2))
            def _():
                line_copy(d, s).wait_recv()
                total = own[d, part, :] + pair_recv[d, part, :] + line[d, part, :].astype(F32)
                line[d, part, :] = total.astype(BF16)
                line_copy(d, s).start()

            @pl.when(place == 3)
            def _():
                line_copy(d, s).wait_recv()
                total = own[d, part, :] + pair_recv[d, part, :] + line[d, part, :].astype(F32)
                gate = total[:, 0:QUARTER]
                up = total[:, QUARTER : 2 * QUARTER]
                back = total[:, 2 * QUARTER : 3 * QUARTER]
                inside = pl.ds(pl.multiple_of((s % PER) * SUB, SUB), SUB)
                prob = rows[s // PER, inside, lanes : lanes + 128].astype(F32)
                prob = jnp.concatenate([prob, prob], axis=1)
                sig = jax.nn.sigmoid(gate)
                hidden = (gate * sig * up).astype(BF16)
                grad = prob * back
                q = 2 * d + core
                hid[q, part, 0:QUARTER] = hidden
                hid[q, part, QUARTER : 2 * QUARTER] = (
                    grad * up * sig * (1.0 + gate * (1.0 - sig))
                ).astype(BF16)
                hid[q, part, 2 * QUARTER : 3 * QUARTER] = (grad * gate * sig).astype(BF16)
                term = jnp.sum(hidden.astype(F32) * back, axis=1, keepdims=True)
                cast_copy(d, s).start()
                core_copy(d, s).start()
                term_send[s] = two_parts(term, SUB)
                zi, _, step = chunk_place(s // PER, s % PER)
                self_too = (s % PER == 0) & (step == 0)

                @pl.when(self_too)
                def _():
                    term_recv[zi, here] = term_send[s]

                @pl.when(jnp.logical_not(self_too))
                def _():
                    term_copy(s).start()

    def term_copy(s):
        zi, to_y, step = chunk_place(s // PER, s % PER)
        return remote(
            term_send.at[s],
            term_recv.at[zi, here],
            term_s.at[0],
            term_r.at[zi],
            at(to_y, zh, (x + step) % 4),
        )

    def two_parts(term, n):
        high = term.astype(BF16).astype(F32)
        lane = lax.broadcasted_iota(jnp.int32, (n, 128), 1)
        return jnp.where(lane < 64, high, term - high).astype(BF16)

    def spread(d, s):
        place = 3 - zl if d == 0 else zl

        @pl.when((s >= 0) & (s < NSUB) & (place < 3))
        def _():
            cast_copy(d, s).wait_recv()

            @pl.when(place > 0)
            def _():
                cast_copy(d, s).start()

            core_copy(d, s).start()

    def chunk_place(k, g):
        zi = jnp.where((k >= 3) & (k < 7), 1, 0)
        late = (k == 2) | (k == 6)
        near = late | (k == 1) | (k == 4)
        far = (k == 5) | (k == 7)
        step = jnp.where(near, jnp.where(g < 2, 3, 1), jnp.where(far, 2, 0))
        source = jnp.where(near, g % 2 + jnp.where(late, 2, 0), g)
        return zi, (y + offset(source)) % 4, step

    def ret_copy(k, g):
        zi, to_y, step = chunk_place(k, g)
        return remote(
            ret_send.at[k, group(g)],
            ret_recv.at[zi, here],
            ret_s.at[0],
            ret_r.at[zi],
            at(to_y, zh, (x + step) % 4),
        )

    def ret_wait(zi):
        part = ret_recv.at[zi, pl.ds(0, 15)]
        remote(part, part, ret_s.at[0], ret_r.at[zi], other_z).wait_recv()

    def back(k, lo=0, n=ROWS):
        for d in range(2):
            for h in range(2):
                if lo <= h * (ROWS // 2) < lo + n:
                    core_wait(d, 2 * k + h)

        take = pl.ds(lo, n)
        part = pl.ds(pl.multiple_of(k * ROWS + lo, ROWS // 2), n)
        total = dot_nt(hid[0, part, QUARTER : 3 * QUARTER], w_in[0])
        for q in range(1, 4):
            total += dot_nt(hid[q, part, QUARTER : 3 * QUARTER], w_in[q])
        ret_send[k, take, :] = total.astype(BF16)
        zi, _, step = chunk_place(k, 0)
        for g in (3, 1, 2):
            if lo <= g * CAP < lo + n:
                ret_copy(k, g).start()

        if lo == 0:

            @pl.when(step != 0)
            def _():
                ret_copy(k, 0).start()

            @pl.when(step == 0)
            def _():
                ret_recv[zi, here] = ret_send[k, 0:CAP, :]

    def weights_in(j):
        two = pl.ds(2 * j, 2)
        turned[...] = rows[two, :, 0:width].reshape(2 * ROWS, width).T
        prob = rows[two, :, lanes : lanes + 128].reshape(2 * ROWS, 128).astype(F32)
        grads = rows[two, :, width:lanes].reshape(2 * ROWS, width).astype(F32)
        scaled[...] = (grads * jnp.concatenate([prob] * (width // 128), axis=1)).astype(BF16)

    def weights(j, q):
        part = pl.ds(pl.multiple_of(2 * j * ROWS, 2 * ROWS), 2 * ROWS)
        up = dot(turned[...], hid[q, part, QUARTER : 3 * QUARTER])
        down = dot_tn(hid[q, part, 0:QUARTER], scaled[...])

        @pl.when(j == 0)
        def _():
            acc_in[q] = up
            acc_out[q] = down

        @pl.when((j > 0) & (j < CHUNKS // 2 - 1))
        def _():
            acc_in[q] += up
            acc_out[q] += down

        @pl.when(j == CHUNKS // 2 - 1)
        def _():
            cols = pl.ds(pl.multiple_of(q * QUARTER, QUARTER), QUARTER)
            out_g[:, cols] = (acc_in[q, :, 0:QUARTER] + up[:, 0:QUARTER]).astype(BF16)
            out_u[:, cols] = (acc_in[q, :, QUARTER : 2 * QUARTER] + up[:, QUARTER : 2 * QUARTER]).astype(BF16)
            out_d[cols, :] = (acc_out[q] + down).astype(BF16)

    choose(0, tok_ref[...], grad_ref[...], ids_ref[...], prob_ref[...].astype(F32))
    place_own(0)
    pltpu.make_async_copy(w_in, w_in, w_sem.at[0]).wait()
    pltpu.make_async_copy(w_out, w_out, w_sem.at[1]).wait()
    project(0, *PARTS[0])
    pl.semaphore_wait(barrier, 23)
    deal(0)
    for d in range(2):
        pair_copy(d, 0, *PARTS[0]).start()
    for copy in raw:
        copy.start()

    def chosen(zi):
        p = p_all[zi]
        first = jnp.where(p > 0.0, 1.0, 0.0).astype(BF16)
        second = jnp.where(p < 0.0, 1.0, 0.0).astype(BF16)
        for i in range(16):
            part = pl.ds(i * CAP, CAP)
            e = (i // 4) * CAP
            pick[0, part, :] = first[e : e + CAP, :]
            pick[1, part, :] = second[e : e + CAP, :]

    def collect(zi):
        ret_wait(zi)
        chosen(zi)
        return dot_tn(pick[0] + pick[1], ret_recv[zi].reshape(16 * CAP, width))

    def collect_terms(zi):
        part = term_recv.at[zi, pl.ds(0, 15)]
        remote(part, part, term_s.at[0], term_r.at[zi], other_z).wait_recv()
        chosen(zi)
        got = term_recv[zi].reshape(16 * CAP, 128)
        terms = [dot_tn(got, pick[i]) for i in range(2)]
        terms = [t[0:1, :] + t[64:65, :] for t in terms]
        return jnp.concatenate(terms, axis=0)

    slot = jnp.where(zl == 3, 2, 0) + core

    def all_copy(o):
        return remote(
            term_all.at[slot],
            term_all.at[slot],
            all_s.at[0],
            all_r.at[0],
            (dp, (tensor + o) % 8),
        )

    last = remote(z_send, z_recv, last_s.at[0], last_r.at[0], other_z)
    last_term = remote(t_send, t_recv, last_s.at[1], last_r.at[1], other_z)

    up_end = 6 * LAG

    def tick(t, carry):
        for d in range(2):
            place = 3 - zl if d == 0 else zl
            spread(d, t - 3 * LAG - LAG * (3 - place))
        for d in range(2):
            place = 3 - zl if d == 0 else zl
            reduce(d, t - LAG * place)

        @pl.when(t == 0)
        def _():
            x_pass(0, (1, 2))
            project(0, *PARTS[1])

        @pl.when(t == 2)
        def _():
            x_pass(0, (3,))
            project(0, *PARTS[2])
            for copy in raw:
                copy.wait_recv()
            choose(1, x_other[0], x_other[1], ids_other[...], prob_other[...].astype(F32))
            place_own(1)
            deal(1)

        @pl.when(t == 2 * PER)
        def _():
            x_pass(1, (1, 2, 3))

        @pl.when(t == 4 * PER)
        def _():
            x_wait(1, 1)
            far_copy(3).start()

        @pl.when((t % PER == PER - 1) & (t + 1 < NSUB))
        def _():
            k = (t + 1) // PER

            @pl.when(k == 1)
            def _():
                x_wait(0, 0)
                far_copy(0).start()

            @pl.when(k == 2)
            def _():
                x_wait(0, 1)
                far_copy(1).start()

            @pl.when(k == 4)
            def _():
                x_wait(1, 0)
                far_copy(2).start()

            @pl.when(k == 5)
            def _():
                far_wait(1)

            @pl.when(k == 7)
            def _():
                far_wait(0)

            project(k)

        u = t - up_end

        @pl.when((u >= PER) & (u % PER == 0) & (u < 8 * PER))
        def _():
            back(u // PER - 1)

        @pl.when(u == 8 * PER - 2)
        def _():
            back(CHUNKS - 1, 0, ROWS // 2)

        v = u - 2 * PER
        j, m = v // (2 * PER), v % (2 * PER)

        @pl.when((v > 0) & (v < 5 * PER) & ((m == 1) | (m == 2) | (m == 5) | (m == 6)))
        def _():
            q = jnp.where(m < 3, m - 1, m - 3)

            @pl.when(q == 0)
            def _():
                weights_in(j)

            weights(j, q)

        @pl.when(u == 8 * PER)
        def _():
            back(CHUNKS - 1, ROWS // 2, ROWS // 2)

        @pl.when((u == TERMS_1) & root)
        def _():
            t_send[...] = collect_terms(1)
            last_term.start()

        @pl.when((u == TERMS_0) & root)
        def _():
            terms = collect_terms(0)
            last_term.wait_recv()
            term_all[slot] = terms + t_recv[...]
            for o in range(1, 8):
                all_copy(o).start()

        @pl.when(u == TURN)
        def _():
            z_send[...] = collect(1).astype(BF16)
            last.start()

        return carry

    lax.fori_loop(0, NSUB + up_end + 1, tick, 0)

    weights(CHUNKS // 2 - 2, 2)
    weights(CHUNKS // 2 - 2, 3)
    weights_in(CHUNKS // 2 - 1)

    def ending(q, carry):
        weights(CHUNKS // 2 - 1, q)
        return carry

    lax.fori_loop(0, 4, ending, 0)
    grads = collect(0)
    last.wait_recv()
    out_x[...] = (grads + z_recv[...].astype(F32)).astype(BF16)

    @pl.when(root)
    def _():
        part = term_all.at[pl.ds(0, 3)]
        remote(part, part, all_s.at[0], all_r.at[0], partner).wait_recv()

    @pl.when(jnp.logical_not(root))
    def _():
        part = term_all.at[pl.ds(0, 4)]
        remote(part, part, all_s.at[0], all_r.at[0], partner).wait_recv()

    out_p[...] = term_all[0] + term_all[1] + term_all[2] + term_all[3]
    last.wait_send()

    @pl.when(root)
    def _():
        last_term.wait_send()
        part = term_all.at[pl.ds(0, 7)]
        remote(part, part, all_s.at[0], all_r.at[0], partner).wait_send()

        part = term_recv.at[:, pl.ds(0, 15)]
        remote(part, part, term_s.at[0], term_r.at[0], other_z).wait_send()

    for copy in raw:
        copy.wait_send()
    for z in range(2):
        part = rows.at[0, pl.ds(0, 3 * CAP)]
        remote(part, part, y_s.at[z], y_r.at[z, 0], other_z).wait_send()
        part = rows.at[pl.ds(0, 2)]
        remote(part, part, x_s.at[z], x_r.at[z, 0], other_z).wait_send()
    part = rows.at[pl.ds(0, 2)]
    remote(part, part, far_s.at[0], far_r.at[0], other_z).wait_send()
    for d in range(2):
        part = pair_recv.at[d]
        remote(part, part, pair_s.at[d], pair_r.at[d, 0], partner).wait_send()
    part = ret_recv.at[:, pl.ds(0, 15)]
    remote(part, part, ret_s.at[0], ret_r.at[0], other_z).wait_send()
    for d in range(2):
        place = 3 - zl if d == 0 else zl
        whole = hid.at[0]

        @pl.when(place < 3)
        def _():
            remote(line.at[d], line.at[d], line_s.at[d], line_r.at[d, 0], partner).wait_send()

        @pl.when(place > 0)
        def _():
            remote(whole, whole, cast_s.at[d], cast_r.at[d, 0], partner).wait_send()

        remote(whole, whole, core_s.at[d], core_r.at[d, 0], partner).wait_send()


def layer(tokens, out_grad, ids, probs, gate_weight, up_weight, down_weight):
    width, hid = gate_weight.shape
    tok = tokens.shape[0]
    total = CHUNKS * ROWS
    vm = pltpu.VMEM
    dma = pltpu.SemaphoreType.DMA
    inner = pl.BlockSpec(memory_space=pltpu.VMEM)
    outer = pl.BlockSpec(memory_space=pl.ANY)
    message = 3 * QUARTER
    return pl.pallas_call(
        functools.partial(kernel, width),
        out_shape=(
            vm((tok, width), BF16),
            vm((2, tok), F32),
            vm((width, hid), BF16),
            vm((width, hid), BF16),
            vm((hid, width), BF16),
        ),
        in_specs=[inner, inner, inner, inner, outer, outer, outer],
        out_specs=(inner,) * 5,
        scratch_shapes=[
            vm((2, tok, width), BF16),
            vm((2, tok), jnp.int32),
            vm((2, tok), BF16),
            vm((2, ROWS, tok), F32),
            vm((CHUNKS, ROWS, 2 * width + 128), BF16),
            vm((2, ROWS, 2 * width + 128), BF16),
            vm((4, width, 2 * QUARTER), BF16),
            vm((hid, width), BF16),
            vm((2, total, message), F32),
            vm((CHUNKS, 2, ROWS, message), F32),
            vm((2, total, message), F32),
            vm((2, total, message), BF16),
            vm((4, total, message), BF16),
            vm((CHUNKS, ROWS, width), BF16),
            vm((2, 16, CAP, width), BF16),
            vm((2, 16 * CAP, tok), BF16),
            vm((tok, width), BF16),
            vm((tok, width), BF16),
            vm((2, tok), F32),
            vm((2, tok), F32),
            vm((4, width, 2 * QUARTER), F32),
            vm((4, QUARTER, width), F32),
            vm((width, 2 * ROWS), BF16),
            vm((2 * ROWS, width), BF16),
            vm((NSUB, CAP, 128), BF16),
            vm((2, 16, CAP, 128), BF16),
            vm((8, 2, tok), F32),
            dma((2,)),
            dma((4,)),
            dma((4,)),
            dma((2,)),
            dma((2, 4)),
            dma((2,)),
            dma((2, 2)),
            dma((1,)),
            dma((2,)),
            dma((2,)),
            dma((2, CHUNKS + 2)),
            dma((2,)),
            dma((2, NSUB)),
            dma((2,)),
            dma((2, NSUB)),
            dma((2,)),
            dma((2, 2 * CHUNKS)),
            dma((1,)),
            dma((2,)),
            dma((2,)),
            dma((2,)),
            dma((1,)),
            dma((2,)),
            dma((1,)),
            dma((1,)),
        ],
        compiler_params=pltpu.CompilerParams(
            collective_id=0, has_side_effects=True, vmem_limit_bytes=55 * 1024 * 1024
        ),
    )(tokens, out_grad, ids, probs, gate_weight, up_weight, down_weight)


def spill(*refs):
    n = len(refs) // 2
    sems = refs[-1]
    copies = [pltpu.make_async_copy(refs[i], refs[n + i], sems.at[i]) for i in range(n)]
    for copy in copies:
        copy.start()
    for copy in copies:
        copy.wait()


def put(arrays):
    return pl.pallas_call(
        spill,
        out_shape=tuple(pltpu.HBM(a.shape, a.dtype) for a in arrays),
        in_specs=[pl.BlockSpec(memory_space=pltpu.VMEM)] * len(arrays),
        out_specs=(pl.BlockSpec(memory_space=pltpu.HBM),) * len(arrays),
        scratch_shapes=[pltpu.SemaphoreType.DMA((len(arrays),))],
        compiler_params=pltpu.CompilerParams(vmem_limit_bytes=16 * 1024 * 1024),
    )(*arrays)


def body(tokens, out_grad, expert_ids, gate_prob, gate_weight, up_weight, down_weight):
    input_grad, terms, gate_grad, up_grad, down_grad = put(
        layer(tokens, out_grad, expert_ids.T, gate_prob.T, gate_weight, up_weight, down_weight)
    )
    return (input_grad, terms.T, gate_grad, up_grad, down_grad)


def solution(mesh):
    return jax.shard_map(
        body,
        mesh=mesh,
        in_specs=(
            P("dp", "tensor"),
            P("dp", "tensor"),
            P("dp", None),
            P("dp", None),
            P("tensor", "dp"),
            P("tensor", "dp"),
            P("dp", "tensor"),
        ),
        out_specs=(
            P("dp", "tensor"),
            P("dp", None),
            P("tensor", "dp"),
            P("tensor", "dp"),
            P("dp", "tensor"),
        ),
        check_vma=False,
    )
```

```python
import functools

import jax
import jax.numpy as jnp
from jax import lax
from jax.experimental import pallas as pl
from jax.experimental.pallas import tpu as pltpu
from jax.sharding import PartitionSpec as P

EXPERTS = 4
CAP = 32
CHUNKS = 8
ROWS = EXPERTS * CAP
SUB = 32
PER = ROWS // SUB
PARTS = ((0, CAP, 0), (CAP, 2 * CAP, CHUNKS), (3 * CAP, CAP, CHUNKS + 1))
NSUB = CHUNKS * PER
LAG = 2
QUARTER = 256
TERMS_1 = 21
TURN = 29
MESH = pl.DeviceIdType.MESH
F32 = jnp.float32
BF16 = jnp.bfloat16


def dot(a, b):
    return lax.dot_general(a, b, (((1,), (0,)), ((), ())), preferred_element_type=F32)


def dot_nt(a, b):
    return lax.dot_general(a, b, (((1,), (1,)), ((), ())), preferred_element_type=F32)


def dot_tn(a, b):
    return lax.dot_general(a, b, (((0,), (0,)), ((), ())), preferred_element_type=F32)


def kernel(
    width,
    tok_ref,
    grad_ref,
    ids_ref,
    prob_ref,
    wg_ref,
    wu_ref,
    wd_ref,
    out_x,
    out_p,
    out_g,
    out_u,
    out_d,
    x_other,
    ids_other,
    prob_other,
    p_all,
    rows,
    y_send,
    w_in,
    w_out,
    own,
    pair_send,
    pair_recv,
    line,
    hid,
    ret_send,
    ret_recv,
    pick,
    z_send,
    z_recv,
    t_send,
    t_recv,
    acc_in,
    acc_out,
    turned,
    scaled,
    term_send,
    term_recv,
    term_all,
    w_sem,
    z_s,
    z_r,
    y_s,
    y_r,
    x_s,
    x_r,
    far_s,
    far_r,
    pair_s,
    pair_r,
    line_s,
    line_r,
    cast_s,
    cast_r,
    core_s,
    core_r,
    ret_s,
    ret_r,
    last_s,
    last_r,
    term_s,
    term_r,
    all_s,
    all_r,
):
    dp = lax.axis_index("dp")
    tensor = lax.axis_index("tensor")
    y, zh, x = dp // 8, (dp // 4) % 2, dp % 4
    zl, core = tensor // 2, tensor % 2
    here = y * 4 + x
    lanes = 2 * width

    def at(y_, zh_, x_):
        return ((y_ * 2 + zh_) * 4 + x_, tensor)

    def plane(j):
        return at(j // 4, zh, j % 4)

    other_z = at(y, 1 - zh, x)
    partner = (dp, zl * 2 + 1 - core)
    root = (zl == 0) | (zl == 3)
    above = (dp, (tensor + 2) % 8)
    below = (dp, (tensor + 6) % 8)

    def remote(src, dst, send, recv, device):
        return pltpu.make_async_remote_copy(
            src_ref=src, dst_ref=dst, send_sem=send, recv_sem=recv, device_id=device, device_id_type=MESH
        )

    barrier = pltpu.get_barrier_semaphore()
    pl.semaphore_signal(barrier, inc=1, device_id=other_z, device_id_type=MESH)
    for o in range(1, 16):
        pl.semaphore_signal(barrier, inc=1, device_id=plane((here + o) % 16), device_id_type=MESH)
    for o in range(1, 8):
        pl.semaphore_signal(barrier, inc=1, device_id=(dp, (tensor + o) % 8), device_id_type=MESH)

    for q in range(4):
        cols = pl.ds(q * QUARTER, QUARTER)
        for i, ref in ((0, wg_ref), (1, wu_ref)):
            pltpu.make_async_copy(
                ref.at[:, cols], w_in.at[q, :, pl.ds(i * QUARTER, QUARTER)], w_sem.at[0]
            ).start()
    pltpu.make_async_copy(wd_ref, w_out, w_sem.at[1]).start()

    raw = [
        remote(ids_ref, ids_other, z_s.at[0], z_r.at[0], other_z),
        remote(prob_ref, prob_other, z_s.at[1], z_r.at[1], other_z),
        remote(tok_ref, x_other.at[0], z_s.at[2], z_r.at[2], other_z),
        remote(grad_ref, x_other.at[1], z_s.at[3], z_r.at[3], other_z),
    ]

    def offset(g):
        return jnp.where(g == 2, 3, jnp.where(g == 3, 2, g))

    def group(g):
        return pl.ds(g * CAP, CAP)

    def y_copy(z, o):
        to = (y + o) % 4
        g = (None, 2, 3, 1)[o]
        return remote(
            y_send.at[z, pl.ds(to * CAP, CAP)],
            rows.at[2 * z, group(g)],
            y_s.at[z],
            y_r.at[z, g],
            at(to, zh, x),
        )

    def y_wait(z, g):
        part = rows.at[2 * z, group(g)]
        remote(part, part, y_s.at[z], y_r.at[z, g], other_z).wait_recv()

    def choose(z, toks, grads, ids, probs):
        count = ids.shape[1]
        named = lax.broadcasted_iota(jnp.int32, (8, count), 0)
        member = jnp.where((named == ids[0:1, :]) | (named == ids[1:2, :]), 1.0, 0.0)
        earlier = jnp.where(
            lax.broadcasted_iota(jnp.int32, (count, count), 0)
            < lax.broadcasted_iota(jnp.int32, (count, count), 1),
            1.0,
            0.0,
        )
        before = dot(member.astype(BF16), earlier.astype(BF16))
        slot = lax.broadcasted_iota(jnp.int32, (CAP, count), 0).astype(F32)
        for e in range(EXPERTS):
            value = jnp.where(ids[0:1, :] == e, probs[0:1, :], -probs[1:2, :])
            value = jnp.where(member[e : e + 1, :] > 0.0, value, 0.0)
            p_all[z, e * CAP : (e + 1) * CAP, :] = jnp.where(slot == before[e : e + 1, :], value, 0.0)
        p = p_all[z]
        one = jnp.where(p != 0.0, 1.0, 0.0).astype(BF16)
        prob = jnp.sum(jnp.abs(p), axis=1, keepdims=True)
        y_send[z, :, 0:width] = dot(one, toks).astype(BF16)
        y_send[z, :, width:lanes] = dot(one, grads).astype(BF16)
        y_send[z, :, lanes : lanes + 128] = jnp.broadcast_to(prob, (ROWS, 128)).astype(BF16)

    def place_own(z):
        rows[2 * z, 0:CAP, :] = y_send[z, pl.ds(pl.multiple_of(y * CAP, CAP), CAP), :]

    def deal(z):
        for o in (1, 3, 2):
            y_copy(z, o).start()
        for side in range(2):
            x_copy(z, side, 0).start()

    right, left = at(y, zh, (x + 1) % 4), at(y, zh, (x + 3) % 4)
    half = ROWS // 2

    def x_copy(z, side, g):
        dst = ((1, 7), (3, 5))[z][g // 2]
        return remote(
            rows.at[2 * z, group(g)],
            rows.at[dst, group(2 * side + g if g < 2 else 2 * (3 - g) + side)],
            x_s.at[z],
            x_r.at[z, g // 2],
            (right, left)[side],
        )

    def x_pass(z, gs):
        for g in gs:
            y_wait(z, g)
            for side in range(2):
                x_copy(z, side, g).start()

    def x_wait(z, h):
        part = rows.at[0]
        remote(part, part, x_s.at[z], x_r.at[z, h], other_z).wait_recv()

    def far_copy(i):
        moves = (
            ((1, 0, 6, 0, half),),
            ((7, 3 * CAP, 6, 2 * CAP, CAP), (7, CAP, 6, 3 * CAP, CAP)),
            ((3, 0, 4, 0, half),),
            ((5, 3 * CAP, 4, 2 * CAP, CAP), (5, CAP, 4, 3 * CAP, CAP)),
        )[i]
        for src, at_src, dst, at_dst, n in moves:
            remote(
                rows.at[src, pl.ds(at_src, n)],
                rows.at[dst, pl.ds(at_dst, n)],
                far_s.at[0],
                far_r.at[i // 2],
                (right, left)[i % 2],
            ).start()

    def far_wait(h):
        part = rows.at[0]
        remote(part, part, far_s.at[0], far_r.at[h], other_z).wait_recv()

    def pair_copy(d, k, lo=0, n=ROWS, i=None):
        i = k if i is None else i
        return remote(
            pair_send.at[k, d, pl.ds(lo, n)],
            pair_recv.at[d, pl.ds(k * ROWS + lo, n)],
            pair_s.at[d],
            pair_r.at[d, i],
            partner,
        )

    def sub_rows(s):
        return pl.ds(pl.multiple_of(s * SUB, SUB), SUB)

    def line_copy(d, s):
        part = line.at[d, sub_rows(s)]
        return remote(part, part, line_s.at[d], line_r.at[d, s], below if d == 0 else above)

    def cast_copy(d, s):
        part = hid.at[2 * d + core, sub_rows(s)]
        return remote(part, part, cast_s.at[d], cast_r.at[d, s], above if d == 0 else below)

    def core_copy(d, s):
        part = hid.at[2 * d + core, sub_rows(s)]
        return remote(part, part, core_s.at[d], core_r.at[d, s // (PER // 2)], partner)

    def core_wait(d, h):
        part = hid.at[2 * d + 1 - core, pl.ds(pl.multiple_of(h * ROWS // 2, ROWS // 2), ROWS // 2)]
        remote(part, part, core_s.at[d], core_r.at[d, h], partner).wait_recv()

    def project(k, lo=0, n=ROWS, i=None):
        take = pl.ds(lo, n)
        for d in range(2):
            for mine in (False, True):
                q = 2 * d + (core if mine else 1 - core)
                up = dot(rows[k, take, 0:width], w_in[q])
                back = dot_nt(
                    rows[k, take, width:lanes],
                    w_out[pl.ds(pl.multiple_of(q * QUARTER, QUARTER), QUARTER), :],
                )
                if mine:
                    part = pl.ds(pl.multiple_of(k * ROWS + lo, CAP), n)
                    own[d, part, 0 : 2 * QUARTER] = up
                    own[d, part, 2 * QUARTER : 3 * QUARTER] = back
                else:
                    pair_send[k, d, take, 0 : 2 * QUARTER] = up
                    pair_send[k, d, take, 2 * QUARTER : 3 * QUARTER] = back
                    if i != 0:
                        pair_copy(d, k, lo, n, i).start()

    def reduce(d, s):
        place = 3 - zl if d == 0 else zl

        @pl.when((s >= 0) & (s < NSUB))
        def _():
            @pl.when((s % PER == 0) & (s > 0))
            def _():
                pair_copy(d, s // PER).wait_recv()

            for lo, n, i in PARTS:

                @pl.when(s == lo // SUB)
                def _():
                    pair_copy(d, 0, lo, n, i).wait_recv()

            part = sub_rows(s)

            @pl.when(place == 0)
            def _():
                line[d, part, :] = (own[d, part, :] + pair_recv[d, part, :]).astype(BF16)
                line_copy(d, s).start()

            @pl.when((place == 1) | (place == 2))
            def _():
                line_copy(d, s).wait_recv()
                total = own[d, part, :] + pair_recv[d, part, :] + line[d, part, :].astype(F32)
                line[d, part, :] = total.astype(BF16)
                line_copy(d, s).start()

            @pl.when(place == 3)
            def _():
                line_copy(d, s).wait_recv()
                total = own[d, part, :] + pair_recv[d, part, :] + line[d, part, :].astype(F32)
                gate = total[:, 0:QUARTER]
                up = total[:, QUARTER : 2 * QUARTER]
                back = total[:, 2 * QUARTER : 3 * QUARTER]
                inside = pl.ds(pl.multiple_of((s % PER) * SUB, SUB), SUB)
                prob = rows[s // PER, inside, lanes : lanes + 128].astype(F32)
                prob = jnp.concatenate([prob, prob], axis=1)
                sig = jax.nn.sigmoid(gate)
                hidden = (gate * sig * up).astype(BF16)
                grad = prob * back
                q = 2 * d + core
                hid[q, part, 0:QUARTER] = hidden
                hid[q, part, QUARTER : 2 * QUARTER] = (
                    grad * up * sig * (1.0 + gate * (1.0 - sig))
                ).astype(BF16)
                hid[q, part, 2 * QUARTER : 3 * QUARTER] = (grad * gate * sig).astype(BF16)
                term = jnp.sum(hidden.astype(F32) * back, axis=1, keepdims=True)
                cast_copy(d, s).start()
                core_copy(d, s).start()
                term_send[s] = two_parts(term, SUB)
                zi, _, step = chunk_place(s // PER, s % PER)
                self_too = (s % PER == 0) & (step == 0)

                @pl.when(self_too)
                def _():
                    term_recv[zi, here] = term_send[s]

                @pl.when(jnp.logical_not(self_too))
                def _():
                    term_copy(s).start()

    def term_copy(s):
        zi, to_y, step = chunk_place(s // PER, s % PER)
        return remote(
            term_send.at[s],
            term_recv.at[zi, here],
            term_s.at[0],
            term_r.at[zi],
            at(to_y, zh, (x + step) % 4),
        )

    def two_parts(term, n):
        high = term.astype(BF16).astype(F32)
        lane = lax.broadcasted_iota(jnp.int32, (n, 128), 1)
        return jnp.where(lane < 64, high, term - high).astype(BF16)

    def spread(d, s):
        place = 3 - zl if d == 0 else zl

        @pl.when((s >= 0) & (s < NSUB) & (place < 3))
        def _():
            cast_copy(d, s).wait_recv()

            @pl.when(place > 0)
            def _():
                cast_copy(d, s).start()

            core_copy(d, s).start()

    def chunk_place(k, g):
        zi = jnp.where((k >= 2) & (k < 6), 1, 0)
        late = (k == 5) | (k == 7)
        near = late | (k == 1) | (k == 3)
        far = (k == 4) | (k == 6)
        side = jnp.where(late, g % 2, g // 2)
        step = jnp.where(near, jnp.where(side == 0, 3, 1), jnp.where(far, 2, 0))
        source = jnp.where(near, jnp.where(late, 3 - g // 2, g % 2), g)
        return zi, (y + offset(source)) % 4, step

    def ret_copy(k, g):
        zi, to_y, step = chunk_place(k, g)
        return remote(
            ret_send.at[k, group(g)],
            ret_recv.at[zi, here],
            ret_s.at[0],
            ret_r.at[zi],
            at(to_y, zh, (x + step) % 4),
        )

    def ret_wait(zi):
        part = ret_recv.at[zi, pl.ds(0, 15)]
        remote(part, part, ret_s.at[0], ret_r.at[zi], other_z).wait_recv()

    def back(k, lo=0, n=ROWS):
        for d in range(2):
            for h in range(2):
                if lo <= h * (ROWS // 2) < lo + n:
                    core_wait(d, 2 * k + h)

        take = pl.ds(lo, n)
        part = pl.ds(pl.multiple_of(k * ROWS + lo, ROWS // 2), n)
        total = dot_nt(hid[0, part, QUARTER : 3 * QUARTER], w_in[0])
        for q in range(1, 4):
            total += dot_nt(hid[q, part, QUARTER : 3 * QUARTER], w_in[q])
        ret_send[k, take, :] = total.astype(BF16)
        zi, _, step = chunk_place(k, 0)
        for g in (2, 3, 1):
            if lo <= g * CAP < lo + n:
                ret_copy(k, g).start()

        if lo == 0:

            @pl.when(step != 0)
            def _():
                ret_copy(k, 0).start()

            @pl.when(step == 0)
            def _():
                ret_recv[zi, here] = ret_send[k, 0:CAP, :]

    def weights_in(j):
        two = pl.ds(2 * j, 2)
        turned[...] = rows[two, :, 0:width].reshape(2 * ROWS, width).T
        prob = rows[two, :, lanes : lanes + 128].reshape(2 * ROWS, 128).astype(F32)
        grads = rows[two, :, width:lanes].reshape(2 * ROWS, width).astype(F32)
        scaled[...] = (grads * jnp.concatenate([prob] * (width // 128), axis=1)).astype(BF16)

    def weights(j, q):
        part = pl.ds(pl.multiple_of(2 * j * ROWS, 2 * ROWS), 2 * ROWS)
        up = dot(turned[...], hid[q, part, QUARTER : 3 * QUARTER])
        down = dot_tn(hid[q, part, 0:QUARTER], scaled[...])

        @pl.when(j == 0)
        def _():
            acc_in[q] = up
            acc_out[q] = down

        @pl.when((j > 0) & (j < CHUNKS // 2 - 1))
        def _():
            acc_in[q] += up
            acc_out[q] += down

        @pl.when(j == CHUNKS // 2 - 1)
        def _():
            cols = pl.ds(pl.multiple_of(q * QUARTER, QUARTER), QUARTER)
            out_g[:, cols] = (acc_in[q, :, 0:QUARTER] + up[:, 0:QUARTER]).astype(BF16)
            out_u[:, cols] = (acc_in[q, :, QUARTER : 2 * QUARTER] + up[:, QUARTER : 2 * QUARTER]).astype(BF16)
            out_d[cols, :] = (acc_out[q] + down).astype(BF16)

    choose(0, tok_ref[...], grad_ref[...], ids_ref[...], prob_ref[...].astype(F32))
    place_own(0)
    pltpu.make_async_copy(w_in, w_in, w_sem.at[0]).wait()
    pltpu.make_async_copy(w_out, w_out, w_sem.at[1]).wait()
    project(0, *PARTS[0])
    pl.semaphore_wait(barrier, 23)
    deal(0)
    for d in range(2):
        pair_copy(d, 0, *PARTS[0]).start()
    for copy in raw:
        copy.start()

    def chosen(zi):
        p = p_all[zi]
        first = jnp.where(p > 0.0, 1.0, 0.0).astype(BF16)
        second = jnp.where(p < 0.0, 1.0, 0.0).astype(BF16)
        for i in range(16):
            part = pl.ds(i * CAP, CAP)
            e = (i // 4) * CAP
            pick[0, part, :] = first[e : e + CAP, :]
            pick[1, part, :] = second[e : e + CAP, :]

    def collect(zi):
        ret_wait(zi)
        chosen(zi)
        return dot_tn(pick[0] + pick[1], ret_recv[zi].reshape(16 * CAP, width))

    def collect_terms(zi):
        part = term_recv.at[zi, pl.ds(0, 15)]
        remote(part, part, term_s.at[0], term_r.at[zi], other_z).wait_recv()
        chosen(zi)
        got = term_recv[zi].reshape(16 * CAP, 128)
        terms = [dot_tn(got, pick[i]) for i in range(2)]
        terms = [t[0:1, :] + t[64:65, :] for t in terms]
        return jnp.concatenate(terms, axis=0)

    slot = jnp.where(zl == 3, 2, 0) + core

    def all_copy(o):
        return remote(
            term_all.at[slot],
            term_all.at[slot],
            all_s.at[0],
            all_r.at[0],
            (dp, (tensor + o) % 8),
        )

    last = remote(z_send, z_recv, last_s.at[0], last_r.at[0], other_z)
    last_term = remote(t_send, t_recv, last_s.at[1], last_r.at[1], other_z)

    up_end = 6 * LAG

    def tick(t, carry):
        for d in range(2):
            place = 3 - zl if d == 0 else zl
            spread(d, t - 3 * LAG - LAG * (3 - place))
        for d in range(2):
            place = 3 - zl if d == 0 else zl
            reduce(d, t - LAG * place)

        @pl.when(t == 0)
        def _():
            x_pass(0, (1, 2))
            project(0, *PARTS[1])

        @pl.when(t == 2)
        def _():
            x_pass(0, (3,))
            project(0, *PARTS[2])

        @pl.when(t == PER + 1)
        def _():
            x_wait(0, 1)
            far_copy(1)

        @pl.when(t == 3 * PER)
        def _():
            x_wait(1, 1)
            far_copy(3)

        @pl.when((t % PER == PER - 1) & (t + 1 < NSUB))
        def _():
            k = (t + 1) // PER

            @pl.when(k == 1)
            def _():
                x_wait(0, 0)
                far_copy(0)

            @pl.when(k == 2)
            def _():
                x_pass(1, (1, 2, 3))

            @pl.when(k == 3)
            def _():
                x_wait(1, 0)
                far_copy(2)

            @pl.when(k == 4)
            def _():
                far_wait(1)

            @pl.when(k == 6)
            def _():
                far_wait(0)

            project(k)

        @pl.when(t == PER - 1)
        def _():
            for copy in raw:
                copy.wait_recv()
            choose(1, x_other[0], x_other[1], ids_other[...], prob_other[...].astype(F32))
            place_own(1)
            deal(1)

        u = t - up_end

        @pl.when((u >= PER) & (u % PER == 0) & (u < 8 * PER))
        def _():
            back(u // PER - 1)

        @pl.when(u == 8 * PER - 2)
        def _():
            back(CHUNKS - 1, 0, ROWS // 2)

        v = u - 2 * PER
        j, m = v // (2 * PER), v % (2 * PER)

        @pl.when((v > 0) & (v < 5 * PER) & ((m == 1) | (m == 2) | (m == 5) | (m == 6)))
        def _():
            q = jnp.where(m < 3, m - 1, m - 3)

            @pl.when(q == 0)
            def _():
                weights_in(j)

            weights(j, q)

        @pl.when(u == 8 * PER)
        def _():
            back(CHUNKS - 1, ROWS // 2, ROWS // 2)

        @pl.when(u == TURN)
        def _():
            z_send[...] = collect(1).astype(BF16)
            last.start()

        @pl.when((u == TERMS_1) & root)
        def _():
            t_send[...] = collect_terms(1)
            last_term.start()

        return carry

    lax.fori_loop(0, NSUB + up_end + 1, tick, 0)

    @pl.when(root)
    def _():
        terms = collect_terms(0)
        last_term.wait_recv()
        term_all[slot] = terms + t_recv[...]
        for o in range(1, 8):
            all_copy(o).start()

    weights(CHUNKS // 2 - 2, 2)
    weights(CHUNKS // 2 - 2, 3)
    weights_in(CHUNKS // 2 - 1)

    def ending(q, carry):
        weights(CHUNKS // 2 - 1, q)
        return carry

    lax.fori_loop(0, 4, ending, 0)
    grads = collect(0)
    last.wait_recv()
    out_x[...] = (grads + z_recv[...].astype(F32)).astype(BF16)

    @pl.when(root)
    def _():
        part = term_all.at[pl.ds(0, 3)]
        remote(part, part, all_s.at[0], all_r.at[0], partner).wait_recv()

    @pl.when(jnp.logical_not(root))
    def _():
        part = term_all.at[pl.ds(0, 4)]
        remote(part, part, all_s.at[0], all_r.at[0], partner).wait_recv()

    out_p[...] = term_all[0] + term_all[1] + term_all[2] + term_all[3]
    last.wait_send()

    @pl.when(root)
    def _():
        last_term.wait_send()
        part = term_all.at[pl.ds(0, 7)]
        remote(part, part, all_s.at[0], all_r.at[0], partner).wait_send()

        part = term_recv.at[:, pl.ds(0, 15)]
        remote(part, part, term_s.at[0], term_r.at[0], other_z).wait_send()

    for copy in raw:
        copy.wait_send()
    for z in range(2):
        part = rows.at[0, pl.ds(0, 3 * CAP)]
        remote(part, part, y_s.at[z], y_r.at[z, 0], other_z).wait_send()
        part = rows.at[pl.ds(0, 2)]
        remote(part, part, x_s.at[z], x_r.at[z, 0], other_z).wait_send()
    part = rows.at[pl.ds(0, 2)]
    remote(part, part, far_s.at[0], far_r.at[0], other_z).wait_send()
    for d in range(2):
        part = pair_recv.at[d]
        remote(part, part, pair_s.at[d], pair_r.at[d, 0], partner).wait_send()
    part = ret_recv.at[:, pl.ds(0, 15)]
    remote(part, part, ret_s.at[0], ret_r.at[0], other_z).wait_send()
    for d in range(2):
        place = 3 - zl if d == 0 else zl
        whole = hid.at[0]

        @pl.when(place < 3)
        def _():
            remote(line.at[d], line.at[d], line_s.at[d], line_r.at[d, 0], partner).wait_send()

        @pl.when(place > 0)
        def _():
            remote(whole, whole, cast_s.at[d], cast_r.at[d, 0], partner).wait_send()

        remote(whole, whole, core_s.at[d], core_r.at[d, 0], partner).wait_send()


def layer(tokens, out_grad, ids, probs, gate_weight, up_weight, down_weight):
    width, hid = gate_weight.shape
    tok = tokens.shape[0]
    total = CHUNKS * ROWS
    vm = pltpu.VMEM
    dma = pltpu.SemaphoreType.DMA
    inner = pl.BlockSpec(memory_space=pltpu.VMEM)
    outer = pl.BlockSpec(memory_space=pl.ANY)
    message = 3 * QUARTER
    return pl.pallas_call(
        functools.partial(kernel, width),
        out_shape=(
            vm((tok, width), BF16),
            vm((2, tok), F32),
            vm((width, hid), BF16),
            vm((width, hid), BF16),
            vm((hid, width), BF16),
        ),
        in_specs=[inner, inner, inner, inner, outer, outer, outer],
        out_specs=(inner,) * 5,
        scratch_shapes=[
            vm((2, tok, width), BF16),
            vm((2, tok), jnp.int32),
            vm((2, tok), BF16),
            vm((2, ROWS, tok), F32),
            vm((CHUNKS, ROWS, 2 * width + 128), BF16),
            vm((2, ROWS, 2 * width + 128), BF16),
            vm((4, width, 2 * QUARTER), BF16),
            vm((hid, width), BF16),
            vm((2, total, message), F32),
            vm((CHUNKS, 2, ROWS, message), F32),
            vm((2, total, message), F32),
            vm((2, total, message), BF16),
            vm((4, total, message), BF16),
            vm((CHUNKS, ROWS, width), BF16),
            vm((2, 16, CAP, width), BF16),
            vm((2, 16 * CAP, tok), BF16),
            vm((tok, width), BF16),
            vm((tok, width), BF16),
            vm((2, tok), F32),
            vm((2, tok), F32),
            vm((4, width, 2 * QUARTER), F32),
            vm((4, QUARTER, width), F32),
            vm((width, 2 * ROWS), BF16),
            vm((2 * ROWS, width), BF16),
            vm((NSUB, CAP, 128), BF16),
            vm((2, 16, CAP, 128), BF16),
            vm((8, 2, tok), F32),
            dma((2,)),
            dma((4,)),
            dma((4,)),
            dma((2,)),
            dma((2, 4)),
            dma((2,)),
            dma((2, 2)),
            dma((1,)),
            dma((2,)),
            dma((2,)),
            dma((2, CHUNKS + 2)),
            dma((2,)),
            dma((2, NSUB)),
            dma((2,)),
            dma((2, NSUB)),
            dma((2,)),
            dma((2, 2 * CHUNKS)),
            dma((1,)),
            dma((2,)),
            dma((2,)),
            dma((2,)),
            dma((1,)),
            dma((2,)),
            dma((1,)),
            dma((1,)),
        ],
        compiler_params=pltpu.CompilerParams(
            collective_id=0, has_side_effects=True, vmem_limit_bytes=55 * 1024 * 1024
        ),
    )(tokens, out_grad, ids, probs, gate_weight, up_weight, down_weight)


def spill(*refs):
    n = len(refs) // 2
    sems = refs[-1]
    copies = [pltpu.make_async_copy(refs[i], refs[n + i], sems.at[i]) for i in range(n)]
    for copy in copies:
        copy.start()
    for copy in copies:
        copy.wait()


def put(arrays):
    return pl.pallas_call(
        spill,
        out_shape=tuple(pltpu.HBM(a.shape, a.dtype) for a in arrays),
        in_specs=[pl.BlockSpec(memory_space=pltpu.VMEM)] * len(arrays),
        out_specs=(pl.BlockSpec(memory_space=pltpu.HBM),) * len(arrays),
        scratch_shapes=[pltpu.SemaphoreType.DMA((len(arrays),))],
        compiler_params=pltpu.CompilerParams(vmem_limit_bytes=16 * 1024 * 1024),
    )(*arrays)


def body(tokens, out_grad, expert_ids, gate_prob, gate_weight, up_weight, down_weight):
    input_grad, terms, gate_grad, up_grad, down_grad = put(
        layer(tokens, out_grad, expert_ids.T, gate_prob.T, gate_weight, up_weight, down_weight)
    )
    return (input_grad, terms.T, gate_grad, up_grad, down_grad)


def solution(mesh):
    return jax.shard_map(
        body,
        mesh=mesh,
        in_specs=(
            P("dp", "tensor"),
            P("dp", "tensor"),
            P("dp", None),
            P("dp", None),
            P("tensor", "dp"),
            P("tensor", "dp"),
            P("dp", "tensor"),
        ),
        out_specs=(
            P("dp", "tensor"),
            P("dp", None),
            P("tensor", "dp"),
            P("tensor", "dp"),
            P("dp", "tensor"),
        ),
        check_vma=False,
    )
```

```python
import functools

import jax
import jax.numpy as jnp
from jax import lax
from jax.experimental import pallas as pl
from jax.experimental.pallas import tpu as pltpu
from jax.sharding import PartitionSpec as P

EXPERTS = 4
CAP = 32
CHUNKS = 8
ROWS = EXPERTS * CAP
SUB = 32
PER = ROWS // SUB
PARTS = ((0, CAP, 0), (CAP, 2 * CAP, CHUNKS), (3 * CAP, CAP, CHUNKS + 1))
LATER = ((0, 3 * CAP, 2), (3 * CAP, CAP, CHUNKS + 2))
NSUB = CHUNKS * PER
LAG = 2
CAST = 2
QUARTER = 256
TERMS_1 = 21
TURN = 29
MESH = pl.DeviceIdType.MESH
F32 = jnp.float32
BF16 = jnp.bfloat16


def dot(a, b):
    return lax.dot_general(a, b, (((1,), (0,)), ((), ())), preferred_element_type=F32)


def dot_nt(a, b):
    return lax.dot_general(a, b, (((1,), (1,)), ((), ())), preferred_element_type=F32)


def dot_tn(a, b):
    return lax.dot_general(a, b, (((0,), (0,)), ((), ())), preferred_element_type=F32)


def kernel(
    width,
    tok_ref,
    grad_ref,
    ids_ref,
    prob_ref,
    wg_ref,
    wu_ref,
    wd_ref,
    out_x,
    out_p,
    out_g,
    out_u,
    out_d,
    x_other,
    ids_other,
    prob_other,
    p_all,
    rows,
    y_send,
    w_in,
    w_out,
    own,
    pair_send,
    pair_recv,
    line,
    hid,
    ret_send,
    ret_recv,
    pick,
    z_send,
    z_recv,
    t_send,
    t_recv,
    acc_in,
    acc_out,
    turned,
    scaled,
    term_send,
    term_recv,
    term_all,
    w_sem,
    z_s,
    z_r,
    y_s,
    y_r,
    x_s,
    x_r,
    far_s,
    far_r,
    pair_s,
    pair_r,
    line_s,
    line_r,
    cast_s,
    cast_r,
    core_s,
    core_r,
    ret_s,
    ret_r,
    last_s,
    last_r,
    term_s,
    term_r,
    all_s,
    all_r,
):
    dp = lax.axis_index("dp")
    tensor = lax.axis_index("tensor")
    y, zh, x = dp // 8, (dp // 4) % 2, dp % 4
    zl, core = tensor // 2, tensor % 2
    here = y * 4 + x
    lanes = 2 * width

    def at(y_, zh_, x_):
        return ((y_ * 2 + zh_) * 4 + x_, tensor)

    def plane(j):
        return at(j // 4, zh, j % 4)

    other_z = at(y, 1 - zh, x)
    partner = (dp, zl * 2 + 1 - core)
    root = (zl == 0) | (zl == 3)
    above = (dp, (tensor + 2) % 8)
    below = (dp, (tensor + 6) % 8)

    def remote(src, dst, send, recv, device):
        return pltpu.make_async_remote_copy(
            src_ref=src, dst_ref=dst, send_sem=send, recv_sem=recv, device_id=device, device_id_type=MESH
        )

    barrier = pltpu.get_barrier_semaphore()
    pl.semaphore_signal(barrier, inc=1, device_id=other_z, device_id_type=MESH)
    for o in range(1, 16):
        pl.semaphore_signal(barrier, inc=1, device_id=plane((here + o) % 16), device_id_type=MESH)
    for o in range(1, 8):
        pl.semaphore_signal(barrier, inc=1, device_id=(dp, (tensor + o) % 8), device_id_type=MESH)

    for q in range(4):
        cols = pl.ds(q * QUARTER, QUARTER)
        for i, ref in ((0, wg_ref), (1, wu_ref)):
            pltpu.make_async_copy(
                ref.at[:, cols], w_in.at[q, :, pl.ds(i * QUARTER, QUARTER)], w_sem.at[0]
            ).start()
    pltpu.make_async_copy(wd_ref, w_out, w_sem.at[1]).start()

    raw = [
        remote(ids_ref, ids_other, z_s.at[0], z_r.at[0], other_z),
        remote(prob_ref, prob_other, z_s.at[1], z_r.at[1], other_z),
        remote(tok_ref, x_other.at[0], z_s.at[2], z_r.at[2], other_z),
        remote(grad_ref, x_other.at[1], z_s.at[3], z_r.at[3], other_z),
    ]

    def offset(g):
        return jnp.where(g == 2, 3, jnp.where(g == 3, 2, g))

    def group(g):
        return pl.ds(g * CAP, CAP)

    def y_copy(z, o):
        to = (y + o) % 4
        g = (None, 2, 3, 1)[o]
        return remote(
            y_send.at[z, pl.ds(to * CAP, CAP)],
            rows.at[2 * z, group(g)],
            y_s.at[z],
            y_r.at[z, g],
            at(to, zh, x),
        )

    def y_wait(z, g):
        part = rows.at[2 * z, group(g)]
        remote(part, part, y_s.at[z], y_r.at[z, g], other_z).wait_recv()

    def choose(z, toks, grads, ids, probs):
        count = ids.shape[1]
        named = lax.broadcasted_iota(jnp.int32, (8, count), 0)
        member = jnp.where((named == ids[0:1, :]) | (named == ids[1:2, :]), 1.0, 0.0)
        earlier = jnp.where(
            lax.broadcasted_iota(jnp.int32, (count, count), 0)
            < lax.broadcasted_iota(jnp.int32, (count, count), 1),
            1.0,
            0.0,
        )
        before = dot(member.astype(BF16), earlier.astype(BF16))
        slot = lax.broadcasted_iota(jnp.int32, (CAP, count), 0).astype(F32)
        for e in range(EXPERTS):
            value = jnp.where(ids[0:1, :] == e, probs[0:1, :], -probs[1:2, :])
            value = jnp.where(member[e : e + 1, :] > 0.0, value, 0.0)
            p_all[z, e * CAP : (e + 1) * CAP, :] = jnp.where(slot == before[e : e + 1, :], value, 0.0)
        p = p_all[z]
        one = jnp.where(p != 0.0, 1.0, 0.0).astype(BF16)
        prob = jnp.sum(jnp.abs(p), axis=1, keepdims=True)
        y_send[z, :, 0:width] = dot(one, toks).astype(BF16)
        y_send[z, :, width:lanes] = dot(one, grads).astype(BF16)
        y_send[z, :, lanes : lanes + 128] = jnp.broadcast_to(prob, (ROWS, 128)).astype(BF16)

    def place_own(z):
        rows[2 * z, 0:CAP, :] = y_send[z, pl.ds(pl.multiple_of(y * CAP, CAP), CAP), :]

    def deal(z):
        for o in (1, 3, 2) if z == 0 else (1, 3):
            y_copy(z, o).start()
        for side in range(2):
            x_copy(z, side, 0).start()

    right, left = at(y, zh, (x + 1) % 4), at(y, zh, (x + 3) % 4)
    half = ROWS // 2

    def x_copy(z, side, g):
        dst = ((1, 7), (3, 5))[z][g // 2]
        return remote(
            rows.at[2 * z, group(g)],
            rows.at[dst, group(2 * side + g if g < 2 else 2 * (3 - g) + side)],
            x_s.at[z],
            x_r.at[z, g // 2],
            (right, left)[side],
        )

    def x_pass(z, gs):
        for g in gs:
            y_wait(z, g)
            for side in range(2):
                x_copy(z, side, g).start()

    def x_wait(z, h):
        part = rows.at[0]
        remote(part, part, x_s.at[z], x_r.at[z, h], other_z).wait_recv()

    def far_copy(i):
        moves = (
            ((1, 0, 6, 0, half),),
            ((7, 3 * CAP, 6, 2 * CAP, CAP), (7, CAP, 6, 3 * CAP, CAP)),
            ((3, 0, 4, 0, half),),
            ((5, 3 * CAP, 4, 2 * CAP, CAP), (5, CAP, 4, 3 * CAP, CAP)),
        )[i]
        for src, at_src, dst, at_dst, n in moves:
            remote(
                rows.at[src, pl.ds(at_src, n)],
                rows.at[dst, pl.ds(at_dst, n)],
                far_s.at[0],
                far_r.at[i // 2],
                (right, left)[i % 2],
            ).start()

    def far_wait(h):
        part = rows.at[0]
        remote(part, part, far_s.at[0], far_r.at[h], other_z).wait_recv()

    def pair_copy(d, k, lo=0, n=ROWS, i=None):
        i = k if i is None else i
        return remote(
            pair_send.at[k, d, pl.ds(lo, n)],
            pair_recv.at[d, pl.ds(k * ROWS + lo, n)],
            pair_s.at[d],
            pair_r.at[d, i],
            partner,
        )

    def sub_rows(s):
        return pl.ds(pl.multiple_of(s * SUB, SUB), SUB)

    def line_copy(d, s):
        part = line.at[d, sub_rows(s)]
        return remote(part, part, line_s.at[d], line_r.at[d, s], below if d == 0 else above)

    def cast_copy(d, s):
        part = hid.at[2 * d + core, sub_rows(s)]
        return remote(part, part, cast_s.at[d], cast_r.at[d, s], above if d == 0 else below)

    def core_copy(d, s):
        part = hid.at[2 * d + core, sub_rows(s)]
        return remote(part, part, core_s.at[d], core_r.at[d, s // (PER // 2)], partner)

    def core_wait(d, h):
        part = hid.at[2 * d + 1 - core, pl.ds(pl.multiple_of(h * ROWS // 2, ROWS // 2), ROWS // 2)]
        remote(part, part, core_s.at[d], core_r.at[d, h], partner).wait_recv()

    def project(k, lo=0, n=ROWS, i=None):
        take = pl.ds(lo, n)
        for d in range(2):
            for mine in (False, True):
                q = 2 * d + (core if mine else 1 - core)
                up = dot(rows[k, take, 0:width], w_in[q])
                back = dot_nt(
                    rows[k, take, width:lanes],
                    w_out[pl.ds(pl.multiple_of(q * QUARTER, QUARTER), QUARTER), :],
                )
                if mine:
                    part = pl.ds(pl.multiple_of(k * ROWS + lo, CAP), n)
                    own[d, part, 0 : 2 * QUARTER] = up
                    own[d, part, 2 * QUARTER : 3 * QUARTER] = back
                else:
                    pair_send[k, d, take, 0 : 2 * QUARTER] = up
                    pair_send[k, d, take, 2 * QUARTER : 3 * QUARTER] = back
                    if i != 0:
                        pair_copy(d, k, lo, n, i).start()

    def reduce(d, s):
        place = 3 - zl if d == 0 else zl

        @pl.when((s >= 0) & (s < NSUB))
        def _():
            @pl.when((s % PER == 0) & (s > 0) & (s != 2 * PER))
            def _():
                pair_copy(d, s // PER).wait_recv()

            for lo, n, i in LATER:

                @pl.when(s == 2 * PER + lo // SUB)
                def _():
                    pair_copy(d, 2, lo, n, i).wait_recv()

            for lo, n, i in PARTS:

                @pl.when(s == lo // SUB)
                def _():
                    pair_copy(d, 0, lo, n, i).wait_recv()

            part = sub_rows(s)

            @pl.when(place == 0)
            def _():
                line[d, part, :] = (own[d, part, :] + pair_recv[d, part, :]).astype(BF16)
                line_copy(d, s).start()

            @pl.when((place == 1) | (place == 2))
            def _():
                line_copy(d, s).wait_recv()
                total = own[d, part, :] + pair_recv[d, part, :] + line[d, part, :].astype(F32)
                line[d, part, :] = total.astype(BF16)
                line_copy(d, s).start()

            @pl.when(place == 3)
            def _():
                line_copy(d, s).wait_recv()
                total = own[d, part, :] + pair_recv[d, part, :] + line[d, part, :].astype(F32)
                gate = total[:, 0:QUARTER]
                up = total[:, QUARTER : 2 * QUARTER]
                back = total[:, 2 * QUARTER : 3 * QUARTER]
                inside = pl.ds(pl.multiple_of((s % PER) * SUB, SUB), SUB)
                prob = rows[s // PER, inside, lanes : lanes + 128].astype(F32)
                prob = jnp.concatenate([prob, prob], axis=1)
                sig = jax.nn.sigmoid(gate)
                hidden = (gate * sig * up).astype(BF16)
                grad = prob * back
                q = 2 * d + core
                hid[q, part, 0:QUARTER] = hidden
                hid[q, part, QUARTER : 2 * QUARTER] = (
                    grad * up * sig * (1.0 + gate * (1.0 - sig))
                ).astype(BF16)
                hid[q, part, 2 * QUARTER : 3 * QUARTER] = (grad * gate * sig).astype(BF16)
                term = jnp.sum(hidden.astype(F32) * back, axis=1, keepdims=True)
                cast_copy(d, s).start()
                core_copy(d, s).start()
                term_send[s] = two_parts(term, SUB)
                zi, _, step = chunk_place(s // PER, s % PER)
                self_too = (s % PER == 0) & (step == 0)

                @pl.when(self_too)
                def _():
                    term_recv[zi, here] = term_send[s]

                @pl.when(jnp.logical_not(self_too))
                def _():
                    term_copy(s).start()

    def term_copy(s):
        zi, to_y, step = chunk_place(s // PER, s % PER)
        return remote(
            term_send.at[s],
            term_recv.at[zi, here],
            term_s.at[0],
            term_r.at[zi],
            at(to_y, zh, (x + step) % 4),
        )

    def two_parts(term, n):
        high = term.astype(BF16).astype(F32)
        lane = lax.broadcasted_iota(jnp.int32, (n, 128), 1)
        return jnp.where(lane < 64, high, term - high).astype(BF16)

    def spread(d, s):
        place = 3 - zl if d == 0 else zl

        @pl.when((s >= 0) & (s < NSUB) & (place < 3))
        def _():
            cast_copy(d, s).wait_recv()

            @pl.when(place > 0)
            def _():
                cast_copy(d, s).start()

            core_copy(d, s).start()

    def chunk_place(k, g):
        zi = jnp.where((k >= 2) & (k < 6), 1, 0)
        late = (k == 5) | (k == 7)
        near = late | (k == 1) | (k == 3)
        far = (k == 4) | (k == 6)
        side = jnp.where(late, g % 2, g // 2)
        step = jnp.where(near, jnp.where(side == 0, 3, 1), jnp.where(far, 2, 0))
        source = jnp.where(near, jnp.where(late, 3 - g // 2, g % 2), g)
        return zi, (y + offset(source)) % 4, step

    def ret_copy(k, g):
        zi, to_y, step = chunk_place(k, g)
        return remote(
            ret_send.at[k, group(g)],
            ret_recv.at[zi, here],
            ret_s.at[0],
            ret_r.at[zi],
            at(to_y, zh, (x + step) % 4),
        )

    def ret_wait(zi):
        part = ret_recv.at[zi, pl.ds(0, 15)]
        remote(part, part, ret_s.at[0], ret_r.at[zi], other_z).wait_recv()

    def back(k, lo=0, n=ROWS):
        for d in range(2):
            for h in range(2):
                if lo <= h * (ROWS // 2) < lo + n:
                    core_wait(d, 2 * k + h)

        take = pl.ds(lo, n)
        part = pl.ds(pl.multiple_of(k * ROWS + lo, ROWS // 2), n)
        total = dot_nt(hid[0, part, QUARTER : 3 * QUARTER], w_in[0])
        for q in range(1, 4):
            total += dot_nt(hid[q, part, QUARTER : 3 * QUARTER], w_in[q])
        ret_send[k, take, :] = total.astype(BF16)
        zi, _, step = chunk_place(k, 0)
        for g in (2, 3, 1):
            if lo <= g * CAP < lo + n:
                ret_copy(k, g).start()

        if lo == 0:

            @pl.when(step != 0)
            def _():
                ret_copy(k, 0).start()

            @pl.when(step == 0)
            def _():
                ret_recv[zi, here] = ret_send[k, 0:CAP, :]

    def weights_in(j):
        two = pl.ds(2 * j, 2)
        turned[...] = rows[two, :, 0:width].reshape(2 * ROWS, width).T
        prob = rows[two, :, lanes : lanes + 128].reshape(2 * ROWS, 128).astype(F32)
        grads = rows[two, :, width:lanes].reshape(2 * ROWS, width).astype(F32)
        scaled[...] = (grads * jnp.concatenate([prob] * (width // 128), axis=1)).astype(BF16)

    def weights(j, q):
        part = pl.ds(pl.multiple_of(2 * j * ROWS, 2 * ROWS), 2 * ROWS)
        up = dot(turned[...], hid[q, part, QUARTER : 3 * QUARTER])
        down = dot_tn(hid[q, part, 0:QUARTER], scaled[...])

        @pl.when(j == 0)
        def _():
            acc_in[q] = up
            acc_out[q] = down

        @pl.when((j > 0) & (j < CHUNKS // 2 - 1))
        def _():
            acc_in[q] += up
            acc_out[q] += down

        @pl.when(j == CHUNKS // 2 - 1)
        def _():
            cols = pl.ds(pl.multiple_of(q * QUARTER, QUARTER), QUARTER)
            out_g[:, cols] = (acc_in[q, :, 0:QUARTER] + up[:, 0:QUARTER]).astype(BF16)
            out_u[:, cols] = (acc_in[q, :, QUARTER : 2 * QUARTER] + up[:, QUARTER : 2 * QUARTER]).astype(BF16)
            out_d[cols, :] = (acc_out[q] + down).astype(BF16)

    choose(0, tok_ref[...], grad_ref[...], ids_ref[...], prob_ref[...].astype(F32))
    place_own(0)
    pltpu.make_async_copy(w_in, w_in, w_sem.at[0]).wait()
    pltpu.make_async_copy(w_out, w_out, w_sem.at[1]).wait()
    project(0, *PARTS[0])
    pl.semaphore_wait(barrier, 23)
    deal(0)
    for d in range(2):
        pair_copy(d, 0, *PARTS[0]).start()
    for copy in raw:
        copy.start()

    def chosen(zi):
        p = p_all[zi]
        first = jnp.where(p > 0.0, 1.0, 0.0).astype(BF16)
        second = jnp.where(p < 0.0, 1.0, 0.0).astype(BF16)
        for i in range(16):
            part = pl.ds(i * CAP, CAP)
            e = (i // 4) * CAP
            pick[0, part, :] = first[e : e + CAP, :]
            pick[1, part, :] = second[e : e + CAP, :]

    def collect(zi):
        ret_wait(zi)
        chosen(zi)
        return dot_tn(pick[0] + pick[1], ret_recv[zi].reshape(16 * CAP, width))

    def collect_terms(zi):
        part = term_recv.at[zi, pl.ds(0, 15)]
        remote(part, part, term_s.at[0], term_r.at[zi], other_z).wait_recv()
        chosen(zi)
        got = term_recv[zi].reshape(16 * CAP, 128)
        terms = [dot_tn(got, pick[i]) for i in range(2)]
        terms = [t[0:1, :] + t[64:65, :] for t in terms]
        return jnp.concatenate(terms, axis=0)

    slot = jnp.where(zl == 3, 2, 0) + core

    def all_copy(o):
        return remote(
            term_all.at[slot],
            term_all.at[slot],
            all_s.at[0],
            all_r.at[0],
            (dp, (tensor + o) % 8),
        )

    last = remote(z_send, z_recv, last_s.at[0], last_r.at[0], other_z)
    last_term = remote(t_send, t_recv, last_s.at[1], last_r.at[1], other_z)

    up_end = 3 * LAG + 3 * CAST

    def tick(t, carry):
        for d in range(2):
            place = 3 - zl if d == 0 else zl
            spread(d, t - 3 * LAG - CAST * (3 - place))
        for d in range(2):
            place = 3 - zl if d == 0 else zl
            reduce(d, t - LAG * place)

        @pl.when(t == 0)
        def _():
            x_pass(0, (1, 2))
            project(0, *PARTS[1])

        @pl.when(t == 2)
        def _():
            x_pass(0, (3,))
            project(0, *PARTS[2])

        @pl.when(t == PER + 1)
        def _():
            y_copy(1, 2).start()
            x_wait(0, 1)
            far_copy(1)

        @pl.when(t == 3 * PER)
        def _():
            x_wait(1, 1)
            far_copy(3)

        @pl.when(t == 2 * PER - 1)
        def _():
            x_pass(1, (1, 2))
            project(2, *LATER[0])

        @pl.when(t == 2 * PER + 1)
        def _():
            x_pass(1, (3,))
            project(2, *LATER[1])

        @pl.when((t % PER == PER - 1) & (t + 1 < NSUB) & (t != 2 * PER - 1))
        def _():
            k = (t + 1) // PER

            @pl.when(k == 1)
            def _():
                x_wait(0, 0)
                far_copy(0)

            @pl.when(k == 3)
            def _():
                x_wait(1, 0)
                far_copy(2)

            @pl.when(k == 4)
            def _():
                far_wait(1)

            @pl.when(k == 6)
            def _():
                far_wait(0)

            project(k)

        @pl.when(t == PER - 1)
        def _():
            for copy in raw:
                copy.wait_recv()
            choose(1, x_other[0], x_other[1], ids_other[...], prob_other[...].astype(F32))
            place_own(1)
            deal(1)

        u = t - up_end

        @pl.when((u >= PER) & (u % PER == 0) & (u < 8 * PER))
        def _():
            back(u // PER - 1)

        @pl.when(u == 8 * PER - 2)
        def _():
            back(CHUNKS - 1, 0, ROWS // 2)

        v = u - 2 * PER
        j, m = v // (2 * PER), v % (2 * PER)

        @pl.when((v > 0) & (v < 5 * PER) & ((m == 1) | (m == 2) | (m == 5) | (m == 6)))
        def _():
            q = jnp.where(m < 3, m - 1, m - 3)

            @pl.when(q == 0)
            def _():
                weights_in(j)

            weights(j, q)

        @pl.when(u == 8 * PER)
        def _():
            back(CHUNKS - 1, ROWS // 2, ROWS // 2)

        @pl.when(u == TURN)
        def _():
            z_send[...] = collect(1).astype(BF16)
            last.start()

        @pl.when((u == TERMS_1) & root)
        def _():
            t_send[...] = collect_terms(1)
            last_term.start()

        return carry

    lax.fori_loop(0, NSUB + up_end + 1, tick, 0)

    @pl.when(root)
    def _():
        terms = collect_terms(0)
        last_term.wait_recv()
        term_all[slot] = terms + t_recv[...]
        for o in range(1, 8):
            all_copy(o).start()

    weights(CHUNKS // 2 - 2, 2)
    weights(CHUNKS // 2 - 2, 3)
    weights_in(CHUNKS // 2 - 1)

    def ending(q, carry):
        weights(CHUNKS // 2 - 1, q)
        return carry

    lax.fori_loop(0, 4, ending, 0)
    grads = collect(0)
    last.wait_recv()
    out_x[...] = (grads + z_recv[...].astype(F32)).astype(BF16)

    @pl.when(root)
    def _():
        part = term_all.at[pl.ds(0, 3)]
        remote(part, part, all_s.at[0], all_r.at[0], partner).wait_recv()

    @pl.when(jnp.logical_not(root))
    def _():
        part = term_all.at[pl.ds(0, 4)]
        remote(part, part, all_s.at[0], all_r.at[0], partner).wait_recv()

    out_p[...] = term_all[0] + term_all[1] + term_all[2] + term_all[3]
    last.wait_send()

    @pl.when(root)
    def _():
        last_term.wait_send()
        part = term_all.at[pl.ds(0, 7)]
        remote(part, part, all_s.at[0], all_r.at[0], partner).wait_send()

        part = term_recv.at[:, pl.ds(0, 15)]
        remote(part, part, term_s.at[0], term_r.at[0], other_z).wait_send()

    for copy in raw:
        copy.wait_send()
    for z in range(2):
        part = rows.at[0, pl.ds(0, 3 * CAP)]
        remote(part, part, y_s.at[z], y_r.at[z, 0], other_z).wait_send()
        part = rows.at[pl.ds(0, 2)]
        remote(part, part, x_s.at[z], x_r.at[z, 0], other_z).wait_send()
    part = rows.at[pl.ds(0, 2)]
    remote(part, part, far_s.at[0], far_r.at[0], other_z).wait_send()
    for d in range(2):
        part = pair_recv.at[d]
        remote(part, part, pair_s.at[d], pair_r.at[d, 0], partner).wait_send()
    part = ret_recv.at[:, pl.ds(0, 15)]
    remote(part, part, ret_s.at[0], ret_r.at[0], other_z).wait_send()
    for d in range(2):
        place = 3 - zl if d == 0 else zl
        whole = hid.at[0]

        @pl.when(place < 3)
        def _():
            remote(line.at[d], line.at[d], line_s.at[d], line_r.at[d, 0], partner).wait_send()

        @pl.when(place > 0)
        def _():
            remote(whole, whole, cast_s.at[d], cast_r.at[d, 0], partner).wait_send()

        remote(whole, whole, core_s.at[d], core_r.at[d, 0], partner).wait_send()


def layer(tokens, out_grad, ids, probs, gate_weight, up_weight, down_weight):
    width, hid = gate_weight.shape
    tok = tokens.shape[0]
    total = CHUNKS * ROWS
    vm = pltpu.VMEM
    dma = pltpu.SemaphoreType.DMA
    inner = pl.BlockSpec(memory_space=pltpu.VMEM)
    outer = pl.BlockSpec(memory_space=pl.ANY)
    message = 3 * QUARTER
    return pl.pallas_call(
        functools.partial(kernel, width),
        out_shape=(
            vm((tok, width), BF16),
            vm((2, tok), F32),
            vm((width, hid), BF16),
            vm((width, hid), BF16),
            vm((hid, width), BF16),
        ),
        in_specs=[inner, inner, inner, inner, outer, outer, outer],
        out_specs=(inner,) * 5,
        scratch_shapes=[
            vm((2, tok, width), BF16),
            vm((2, tok), jnp.int32),
            vm((2, tok), BF16),
            vm((2, ROWS, tok), F32),
            vm((CHUNKS, ROWS, 2 * width + 128), BF16),
            vm((2, ROWS, 2 * width + 128), BF16),
            vm((4, width, 2 * QUARTER), BF16),
            vm((hid, width), BF16),
            vm((2, total, message), F32),
            vm((CHUNKS, 2, ROWS, message), F32),
            vm((2, total, message), F32),
            vm((2, total, message), BF16),
            vm((4, total, message), BF16),
            vm((CHUNKS, ROWS, width), BF16),
            vm((2, 16, CAP, width), BF16),
            vm((2, 16 * CAP, tok), BF16),
            vm((tok, width), BF16),
            vm((tok, width), BF16),
            vm((2, tok), F32),
            vm((2, tok), F32),
            vm((4, width, 2 * QUARTER), F32),
            vm((4, QUARTER, width), F32),
            vm((width, 2 * ROWS), BF16),
            vm((2 * ROWS, width), BF16),
            vm((NSUB, CAP, 128), BF16),
            vm((2, 16, CAP, 128), BF16),
            vm((8, 2, tok), F32),
            dma((2,)),
            dma((4,)),
            dma((4,)),
            dma((2,)),
            dma((2, 4)),
            dma((2,)),
            dma((2, 2)),
            dma((1,)),
            dma((2,)),
            dma((2,)),
            dma((2, CHUNKS + 3)),
            dma((2,)),
            dma((2, NSUB)),
            dma((2,)),
            dma((2, NSUB)),
            dma((2,)),
            dma((2, 2 * CHUNKS)),
            dma((1,)),
            dma((2,)),
            dma((2,)),
            dma((2,)),
            dma((1,)),
            dma((2,)),
            dma((1,)),
            dma((1,)),
        ],
        compiler_params=pltpu.CompilerParams(
            collective_id=0, has_side_effects=True, vmem_limit_bytes=55 * 1024 * 1024
        ),
    )(tokens, out_grad, ids, probs, gate_weight, up_weight, down_weight)


def spill(*refs):
    n = len(refs) // 2
    sems = refs[-1]
    copies = [pltpu.make_async_copy(refs[i], refs[n + i], sems.at[i]) for i in range(n)]
    for copy in copies:
        copy.start()
    for copy in copies:
        copy.wait()


def put(arrays):
    return pl.pallas_call(
        spill,
        out_shape=tuple(pltpu.HBM(a.shape, a.dtype) for a in arrays),
        in_specs=[pl.BlockSpec(memory_space=pltpu.VMEM)] * len(arrays),
        out_specs=(pl.BlockSpec(memory_space=pltpu.HBM),) * len(arrays),
        scratch_shapes=[pltpu.SemaphoreType.DMA((len(arrays),))],
        compiler_params=pltpu.CompilerParams(vmem_limit_bytes=16 * 1024 * 1024),
    )(*arrays)


def body(tokens, out_grad, expert_ids, gate_prob, gate_weight, up_weight, down_weight):
    input_grad, terms, gate_grad, up_grad, down_grad = put(
        layer(tokens, out_grad, expert_ids.T, gate_prob.T, gate_weight, up_weight, down_weight)
    )
    return (input_grad, terms.T, gate_grad, up_grad, down_grad)


def solution(mesh):
    return jax.shard_map(
        body,
        mesh=mesh,
        in_specs=(
            P("dp", "tensor"),
            P("dp", "tensor"),
            P("dp", None),
            P("dp", None),
            P("tensor", "dp"),
            P("tensor", "dp"),
            P("dp", "tensor"),
        ),
        out_specs=(
            P("dp", "tensor"),
            P("dp", None),
            P("tensor", "dp"),
            P("tensor", "dp"),
            P("dp", "tensor"),
        ),
        check_vma=False,
    )
```

```python
import functools

import jax
import jax.numpy as jnp
from jax import lax
from jax.experimental import pallas as pl
from jax.experimental.pallas import tpu as pltpu
from jax.sharding import PartitionSpec as P

EXPERTS = 4
CAP = 32
CHUNKS = 8
ROWS = EXPERTS * CAP
SUB = 32
PER = ROWS // SUB
PARTS = ((0, CAP, 0), (CAP, 2 * CAP, CHUNKS), (3 * CAP, CAP, CHUNKS + 1))
LATER = ((0, 3 * CAP, 2), (3 * CAP, CAP, CHUNKS + 2))
NSUB = CHUNKS * PER
LAG = 2
CAST = 2
QUARTER = 256
TERMS_1 = 21
TURN = 29
MESH = pl.DeviceIdType.MESH
F32 = jnp.float32
BF16 = jnp.bfloat16


def dot(a, b):
    return lax.dot_general(a, b, (((1,), (0,)), ((), ())), preferred_element_type=F32)


def dot_nt(a, b):
    return lax.dot_general(a, b, (((1,), (1,)), ((), ())), preferred_element_type=F32)


def dot_tn(a, b):
    return lax.dot_general(a, b, (((0,), (0,)), ((), ())), preferred_element_type=F32)


def kernel(
    width,
    tok_ref,
    grad_ref,
    ids_ref,
    prob_ref,
    wg_ref,
    wu_ref,
    wd_ref,
    out_x,
    out_p,
    out_g,
    out_u,
    out_d,
    x_other,
    ids_other,
    prob_other,
    p_all,
    rows,
    y_send,
    w_in,
    w_out,
    own,
    pair_send,
    pair_recv,
    line,
    hid,
    ret_send,
    ret_recv,
    pick,
    z_send,
    z_recv,
    t_send,
    t_recv,
    acc_in,
    acc_out,
    turned,
    scaled,
    term_send,
    term_recv,
    term_all,
    w_sem,
    z_s,
    z_r,
    y_s,
    y_r,
    x_s,
    x_r,
    far_s,
    far_r,
    pair_s,
    pair_r,
    line_s,
    line_r,
    cast_s,
    cast_r,
    core_s,
    core_r,
    ret_s,
    ret_r,
    last_s,
    last_r,
    term_s,
    term_r,
    all_s,
    all_r,
):
    dp = lax.axis_index("dp")
    tensor = lax.axis_index("tensor")
    y, zh, x = dp // 8, (dp // 4) % 2, dp % 4
    zl, core = tensor // 2, tensor % 2
    here = y * 4 + x
    lanes = 2 * width

    def at(y_, zh_, x_):
        return ((y_ * 2 + zh_) * 4 + x_, tensor)

    def plane(j):
        return at(j // 4, zh, j % 4)

    other_z = at(y, 1 - zh, x)
    partner = (dp, zl * 2 + 1 - core)
    root = (zl == 0) | (zl == 3)
    above = (dp, (tensor + 2) % 8)
    below = (dp, (tensor + 6) % 8)

    def remote(src, dst, send, recv, device):
        return pltpu.make_async_remote_copy(
            src_ref=src, dst_ref=dst, send_sem=send, recv_sem=recv, device_id=device, device_id_type=MESH
        )

    barrier = pltpu.get_barrier_semaphore()
    pl.semaphore_signal(barrier, inc=1, device_id=other_z, device_id_type=MESH)
    for o in range(1, 16):
        pl.semaphore_signal(barrier, inc=1, device_id=plane((here + o) % 16), device_id_type=MESH)
    for o in range(1, 8):
        pl.semaphore_signal(barrier, inc=1, device_id=(dp, (tensor + o) % 8), device_id_type=MESH)

    for q in range(4):
        cols = pl.ds(q * QUARTER, QUARTER)
        for i, ref in ((0, wg_ref), (1, wu_ref)):
            pltpu.make_async_copy(
                ref.at[:, cols], w_in.at[q, :, pl.ds(i * QUARTER, QUARTER)], w_sem.at[0]
            ).start()
    pltpu.make_async_copy(wd_ref, w_out, w_sem.at[1]).start()

    raw = [
        remote(ids_ref, ids_other, z_s.at[0], z_r.at[0], other_z),
        remote(prob_ref, prob_other, z_s.at[1], z_r.at[1], other_z),
        remote(tok_ref, x_other.at[0], z_s.at[2], z_r.at[2], other_z),
        remote(grad_ref, x_other.at[1], z_s.at[3], z_r.at[3], other_z),
    ]

    def offset(g):
        return jnp.where(g == 2, 3, jnp.where(g == 3, 2, g))

    def group(g):
        return pl.ds(g * CAP, CAP)

    def y_copy(z, o):
        to = (y + o) % 4
        g = (None, 2, 3, 1)[o]
        return remote(
            y_send.at[z, pl.ds(to * CAP, CAP)],
            rows.at[2 * z, group(g)],
            y_s.at[z],
            y_r.at[z, g],
            at(to, zh, x),
        )

    def y_wait(z, g):
        part = rows.at[2 * z, group(g)]
        remote(part, part, y_s.at[z], y_r.at[z, g], other_z).wait_recv()

    def choose(z, toks, grads, ids, probs):
        count = ids.shape[1]
        named = lax.broadcasted_iota(jnp.int32, (8, count), 0)
        member = jnp.where((named == ids[0:1, :]) | (named == ids[1:2, :]), 1.0, 0.0)
        earlier = jnp.where(
            lax.broadcasted_iota(jnp.int32, (count, count), 0)
            < lax.broadcasted_iota(jnp.int32, (count, count), 1),
            1.0,
            0.0,
        )
        before = dot(member.astype(BF16), earlier.astype(BF16))
        slot = lax.broadcasted_iota(jnp.int32, (CAP, count), 0).astype(F32)
        for e in range(EXPERTS):
            value = jnp.where(ids[0:1, :] == e, probs[0:1, :], -probs[1:2, :])
            value = jnp.where(member[e : e + 1, :] > 0.0, value, 0.0)
            p_all[z, e * CAP : (e + 1) * CAP, :] = jnp.where(slot == before[e : e + 1, :], value, 0.0)
        p = p_all[z]
        one = jnp.where(p != 0.0, 1.0, 0.0).astype(BF16)
        prob = jnp.sum(jnp.abs(p), axis=1, keepdims=True)
        y_send[z, :, 0:width] = dot(one, toks).astype(BF16)
        y_send[z, :, width:lanes] = dot(one, grads).astype(BF16)
        y_send[z, :, lanes : lanes + 128] = jnp.broadcast_to(prob, (ROWS, 128)).astype(BF16)

    def place_own(z):
        rows[2 * z, 0:CAP, :] = y_send[z, pl.ds(pl.multiple_of(y * CAP, CAP), CAP), :]

    def deal(z):
        for o in (1, 3, 2) if z == 0 else (1, 3):
            y_copy(z, o).start()
        for side in range(2):
            x_copy(z, side, 0).start()

    right, left = at(y, zh, (x + 1) % 4), at(y, zh, (x + 3) % 4)
    half = ROWS // 2

    def x_copy(z, side, g):
        dst = ((1, 7), (3, 5))[z][g // 2]
        return remote(
            rows.at[2 * z, group(g)],
            rows.at[dst, group(2 * side + g if g < 2 else 2 * (3 - g) + side)],
            x_s.at[z],
            x_r.at[z, g // 2],
            (right, left)[side],
        )

    def x_pass(z, gs):
        for g in gs:
            y_wait(z, g)
            for side in range(2):
                x_copy(z, side, g).start()

    def x_wait(z, h):
        part = rows.at[0]
        remote(part, part, x_s.at[z], x_r.at[z, h], other_z).wait_recv()

    def far_copy(i):
        moves = (
            ((1, 0, 6, 0, half),),
            ((7, 3 * CAP, 6, 2 * CAP, CAP), (7, CAP, 6, 3 * CAP, CAP)),
            ((3, 0, 4, 0, half),),
            ((5, 3 * CAP, 4, 2 * CAP, CAP), (5, CAP, 4, 3 * CAP, CAP)),
        )[i]
        for src, at_src, dst, at_dst, n in moves:
            remote(
                rows.at[src, pl.ds(at_src, n)],
                rows.at[dst, pl.ds(at_dst, n)],
                far_s.at[0],
                far_r.at[i // 2],
                (right, left)[i % 2],
            ).start()

    def far_wait(h):
        part = rows.at[0]
        remote(part, part, far_s.at[0], far_r.at[h], other_z).wait_recv()

    def pair_copy(d, k, lo=0, n=ROWS, i=None):
        i = k if i is None else i
        return remote(
            pair_send.at[k, d, pl.ds(lo, n)],
            pair_recv.at[d, pl.ds(k * ROWS + lo, n)],
            pair_s.at[d],
            pair_r.at[d, i],
            partner,
        )

    def sub_rows(s):
        return pl.ds(pl.multiple_of(s * SUB, SUB), SUB)

    def line_copy(d, s):
        part = line.at[d, sub_rows(s)]
        return remote(part, part, line_s.at[d], line_r.at[d, s], below if d == 0 else above)

    def cast_copy(d, s):
        part = hid.at[2 * d + core, sub_rows(s)]
        return remote(part, part, cast_s.at[d], cast_r.at[d, s], above if d == 0 else below)

    def core_copy(d, s):
        part = hid.at[2 * d + core, sub_rows(s)]
        return remote(part, part, core_s.at[d], core_r.at[d, s // (PER // 2)], partner)

    def core_wait(d, h):
        part = hid.at[2 * d + 1 - core, pl.ds(pl.multiple_of(h * ROWS // 2, ROWS // 2), ROWS // 2)]
        remote(part, part, core_s.at[d], core_r.at[d, h], partner).wait_recv()

    def project(k, lo=0, n=ROWS, i=None):
        take = pl.ds(lo, n)
        for d in range(2):
            for mine in (False, True):
                q = 2 * d + (core if mine else 1 - core)
                up = dot(rows[k, take, 0:width], w_in[q])
                back = dot_nt(
                    rows[k, take, width:lanes],
                    w_out[pl.ds(pl.multiple_of(q * QUARTER, QUARTER), QUARTER), :],
                )
                if mine:
                    part = pl.ds(pl.multiple_of(k * ROWS + lo, CAP), n)
                    own[d, part, 0 : 2 * QUARTER] = up
                    own[d, part, 2 * QUARTER : 3 * QUARTER] = back
                else:
                    pair_send[k, d, take, 0 : 2 * QUARTER] = up
                    pair_send[k, d, take, 2 * QUARTER : 3 * QUARTER] = back
                    if i != 0:
                        pair_copy(d, k, lo, n, i).start()

    def reduce(d, s):
        place = 3 - zl if d == 0 else zl

        @pl.when((s >= 0) & (s < NSUB))
        def _():
            @pl.when((s % PER == 0) & (s > 0) & (s != 2 * PER))
            def _():
                pair_copy(d, s // PER).wait_recv()

            for lo, n, i in LATER:

                @pl.when(s == 2 * PER + lo // SUB)
                def _():
                    pair_copy(d, 2, lo, n, i).wait_recv()

            for lo, n, i in PARTS:

                @pl.when(s == lo // SUB)
                def _():
                    pair_copy(d, 0, lo, n, i).wait_recv()

            part = sub_rows(s)

            @pl.when(place == 0)
            def _():
                line[d, part, :] = (own[d, part, :] + pair_recv[d, part, :]).astype(BF16)
                line_copy(d, s).start()

            @pl.when((place == 1) | (place == 2))
            def _():
                line_copy(d, s).wait_recv()
                total = own[d, part, :] + pair_recv[d, part, :] + line[d, part, :].astype(F32)
                line[d, part, :] = total.astype(BF16)
                line_copy(d, s).start()

            @pl.when(place == 3)
            def _():
                line_copy(d, s).wait_recv()
                total = own[d, part, :] + pair_recv[d, part, :] + line[d, part, :].astype(F32)
                gate = total[:, 0:QUARTER]
                up = total[:, QUARTER : 2 * QUARTER]
                back = total[:, 2 * QUARTER : 3 * QUARTER]
                inside = pl.ds(pl.multiple_of((s % PER) * SUB, SUB), SUB)
                prob = rows[s // PER, inside, lanes : lanes + 128].astype(F32)
                prob = jnp.concatenate([prob, prob], axis=1)
                sig = jax.nn.sigmoid(gate)
                hidden = (gate * sig * up).astype(BF16)
                grad = prob * back
                q = 2 * d + core
                hid[q, part, 0:QUARTER] = hidden
                hid[q, part, QUARTER : 2 * QUARTER] = (
                    grad * up * sig * (1.0 + gate * (1.0 - sig))
                ).astype(BF16)
                hid[q, part, 2 * QUARTER : 3 * QUARTER] = (grad * gate * sig).astype(BF16)
                term = jnp.sum(hidden.astype(F32) * back, axis=1, keepdims=True)
                cast_copy(d, s).start()
                core_copy(d, s).start()
                term_send[s] = two_parts(term, SUB)
                zi, _, step = chunk_place(s // PER, s % PER)
                self_too = (s % PER == 0) & (step == 0)

                @pl.when(self_too)
                def _():
                    term_recv[zi, here] = term_send[s]

                @pl.when(jnp.logical_not(self_too))
                def _():
                    term_copy(s).start()

    def term_copy(s):
        zi, to_y, step = chunk_place(s // PER, s % PER)
        return remote(
            term_send.at[s],
            term_recv.at[zi, here],
            term_s.at[0],
            term_r.at[zi],
            at(to_y, zh, (x + step) % 4),
        )

    def two_parts(term, n):
        high = term.astype(BF16).astype(F32)
        lane = lax.broadcasted_iota(jnp.int32, (n, 128), 1)
        return jnp.where(lane < 64, high, term - high).astype(BF16)

    def spread(d, s):
        place = 3 - zl if d == 0 else zl

        @pl.when((s >= 0) & (s < NSUB) & (place < 3))
        def _():
            cast_copy(d, s).wait_recv()

            @pl.when(place > 0)
            def _():
                cast_copy(d, s).start()

            core_copy(d, s).start()

    def chunk_place(k, g):
        zi = jnp.where((k >= 2) & (k < 6), 1, 0)
        late = (k == 5) | (k == 7)
        near = late | (k == 1) | (k == 3)
        far = (k == 4) | (k == 6)
        side = jnp.where(late, g % 2, g // 2)
        step = jnp.where(near, jnp.where(side == 0, 3, 1), jnp.where(far, 2, 0))
        source = jnp.where(near, jnp.where(late, 3 - g // 2, g % 2), g)
        return zi, (y + offset(source)) % 4, step

    def ret_copy(k, g):
        zi, to_y, step = chunk_place(k, g)
        return remote(
            ret_send.at[k, group(g)],
            ret_recv.at[zi, here],
            ret_s.at[0],
            ret_r.at[zi],
            at(to_y, zh, (x + step) % 4),
        )

    def ret_wait(zi):
        part = ret_recv.at[zi, pl.ds(0, 15)]
        remote(part, part, ret_s.at[0], ret_r.at[zi], other_z).wait_recv()

    def back(k, lo=0, n=ROWS):
        for d in range(2):
            for h in range(2):
                if lo <= h * (ROWS // 2) < lo + n:
                    core_wait(d, 2 * k + h)

        take = pl.ds(lo, n)
        part = pl.ds(pl.multiple_of(k * ROWS + lo, ROWS // 2), n)
        total = dot_nt(hid[0, part, QUARTER : 3 * QUARTER], w_in[0])
        for q in range(1, 4):
            total += dot_nt(hid[q, part, QUARTER : 3 * QUARTER], w_in[q])
        ret_send[k, take, :] = total.astype(BF16)
        zi, _, step = chunk_place(k, 0)
        for g in (2, 3, 1):
            if lo <= g * CAP < lo + n:
                ret_copy(k, g).start()

        if lo == 0:

            @pl.when(step != 0)
            def _():
                ret_copy(k, 0).start()

            @pl.when(step == 0)
            def _():
                ret_recv[zi, here] = ret_send[k, 0:CAP, :]

    def weights_in(j):
        two = pl.ds(2 * j, 2)
        turned[...] = rows[two, :, 0:width].reshape(2 * ROWS, width).T
        prob = rows[two, :, lanes : lanes + 128].reshape(2 * ROWS, 128).astype(F32)
        grads = rows[two, :, width:lanes].reshape(2 * ROWS, width).astype(F32)
        scaled[...] = (grads * jnp.concatenate([prob] * (width // 128), axis=1)).astype(BF16)

    def weights(j, q):
        part = pl.ds(pl.multiple_of(2 * j * ROWS, 2 * ROWS), 2 * ROWS)
        up = dot(turned[...], hid[q, part, QUARTER : 3 * QUARTER])
        down = dot_tn(hid[q, part, 0:QUARTER], scaled[...])

        @pl.when(j == 0)
        def _():
            acc_in[q] = up
            acc_out[q] = down

        @pl.when((j > 0) & (j < CHUNKS // 2 - 1))
        def _():
            acc_in[q] += up
            acc_out[q] += down

        @pl.when(j == CHUNKS // 2 - 1)
        def _():
            cols = pl.ds(pl.multiple_of(q * QUARTER, QUARTER), QUARTER)
            out_g[:, cols] = (acc_in[q, :, 0:QUARTER] + up[:, 0:QUARTER]).astype(BF16)
            out_u[:, cols] = (acc_in[q, :, QUARTER : 2 * QUARTER] + up[:, QUARTER : 2 * QUARTER]).astype(BF16)
            out_d[cols, :] = (acc_out[q] + down).astype(BF16)

    choose(0, tok_ref[...], grad_ref[...], ids_ref[...], prob_ref[...].astype(F32))
    place_own(0)
    pltpu.make_async_copy(w_in, w_in, w_sem.at[0]).wait()
    pltpu.make_async_copy(w_out, w_out, w_sem.at[1]).wait()
    project(0, *PARTS[0])
    pl.semaphore_wait(barrier, 23)
    deal(0)
    for d in range(2):
        pair_copy(d, 0, *PARTS[0]).start()
    for copy in raw:
        copy.start()

    def chosen(zi):
        p = p_all[zi]
        first = jnp.where(p > 0.0, 1.0, 0.0).astype(BF16)
        second = jnp.where(p < 0.0, 1.0, 0.0).astype(BF16)
        for i in range(16):
            part = pl.ds(i * CAP, CAP)
            e = (i // 4) * CAP
            pick[0, part, :] = first[e : e + CAP, :]
            pick[1, part, :] = second[e : e + CAP, :]

    def collect(zi):
        ret_wait(zi)
        chosen(zi)
        return dot_tn(pick[0] + pick[1], ret_recv[zi].reshape(16 * CAP, width))

    def collect_terms(zi):
        part = term_recv.at[zi, pl.ds(0, 15)]
        remote(part, part, term_s.at[0], term_r.at[zi], other_z).wait_recv()
        chosen(zi)
        got = term_recv[zi].reshape(16 * CAP, 128)
        terms = [dot_tn(got, pick[i]) for i in range(2)]
        terms = [t[0:1, :] + t[64:65, :] for t in terms]
        return jnp.concatenate(terms, axis=0)

    slot = jnp.where(zl == 3, 2, 0) + core

    def all_copy(o):
        return remote(
            term_all.at[slot],
            term_all.at[slot],
            all_s.at[0],
            all_r.at[0],
            (dp, (tensor + o) % 8),
        )

    last = remote(z_send, z_recv, last_s.at[0], last_r.at[0], other_z)
    last_term = remote(t_send, t_recv, last_s.at[1], last_r.at[1], other_z)

    up_end = 3 * LAG + 3 * CAST

    def tick(t, carry):
        for d in range(2):
            place = 3 - zl if d == 0 else zl
            spread(d, t - 3 * LAG - CAST * (3 - place))
        for d in range(2):
            place = 3 - zl if d == 0 else zl
            reduce(d, t - LAG * place)

        @pl.when(t == 0)
        def _():
            x_pass(0, (1, 2))
            project(0, *PARTS[1])

        @pl.when(t == 2)
        def _():
            x_pass(0, (3,))
            project(0, *PARTS[2])

        @pl.when(t == PER + 1)
        def _():
            y_copy(1, 2).start()

        @pl.when(t == 2 * PER + 2)
        def _():
            x_wait(0, 1)
            far_copy(1)

        @pl.when(t == 3 * PER)
        def _():
            x_wait(1, 1)
            far_copy(3)

        @pl.when(t == 2 * PER - 1)
        def _():
            x_pass(1, (1, 2))
            project(2, *LATER[0])

        @pl.when(t == 2 * PER + 1)
        def _():
            x_pass(1, (3,))
            project(2, *LATER[1])

        @pl.when((t % PER == PER - 1) & (t + 1 < NSUB) & (t != 2 * PER - 1))
        def _():
            k = (t + 1) // PER

            @pl.when(k == 1)
            def _():
                x_wait(0, 0)
                far_copy(0)

            @pl.when(k == 3)
            def _():
                x_wait(1, 0)
                far_copy(2)

            @pl.when(k == 4)
            def _():
                far_wait(1)

            @pl.when(k == 6)
            def _():
                far_wait(0)

            project(k)

        @pl.when(t == PER - 1)
        def _():
            for copy in raw:
                copy.wait_recv()
            choose(1, x_other[0], x_other[1], ids_other[...], prob_other[...].astype(F32))
            place_own(1)
            deal(1)

        u = t - up_end

        @pl.when((u >= PER) & (u % PER == 0) & (u < 8 * PER))
        def _():
            back(u // PER - 1)

        @pl.when(u == 8 * PER - 2)
        def _():
            back(CHUNKS - 1, 0, ROWS // 2)

        v = u - 2 * PER
        j, m = v // (2 * PER), v % (2 * PER)

        @pl.when((v > 0) & (v < 5 * PER) & ((m == 1) | (m == 2) | (m == 5) | (m == 6)))
        def _():
            q = jnp.where(m < 3, m - 1, m - 3)

            @pl.when(q == 0)
            def _():
                weights_in(j)

            weights(j, q)

        @pl.when(u == 8 * PER)
        def _():
            back(CHUNKS - 1, ROWS // 2, ROWS // 2)

        @pl.when(u == TURN)
        def _():
            z_send[...] = collect(1).astype(BF16)
            last.start()

        @pl.when((u == TERMS_1) & root)
        def _():
            t_send[...] = collect_terms(1)
            last_term.start()

        return carry

    lax.fori_loop(0, NSUB + up_end + 1, tick, 0)

    @pl.when(root)
    def _():
        terms = collect_terms(0)
        last_term.wait_recv()
        term_all[slot] = terms + t_recv[...]
        for o in range(1, 8):
            all_copy(o).start()

    weights(CHUNKS // 2 - 2, 2)
    weights(CHUNKS // 2 - 2, 3)
    weights_in(CHUNKS // 2 - 1)

    def ending(q, carry):
        weights(CHUNKS // 2 - 1, q)
        return carry

    lax.fori_loop(0, 4, ending, 0)
    grads = collect(0)
    last.wait_recv()
    out_x[...] = (grads + z_recv[...].astype(F32)).astype(BF16)

    @pl.when(root)
    def _():
        part = term_all.at[pl.ds(0, 3)]
        remote(part, part, all_s.at[0], all_r.at[0], partner).wait_recv()

    @pl.when(jnp.logical_not(root))
    def _():
        part = term_all.at[pl.ds(0, 4)]
        remote(part, part, all_s.at[0], all_r.at[0], partner).wait_recv()

    out_p[...] = term_all[0] + term_all[1] + term_all[2] + term_all[3]
    last.wait_send()

    @pl.when(root)
    def _():
        last_term.wait_send()
        part = term_all.at[pl.ds(0, 7)]
        remote(part, part, all_s.at[0], all_r.at[0], partner).wait_send()

        part = term_recv.at[:, pl.ds(0, 15)]
        remote(part, part, term_s.at[0], term_r.at[0], other_z).wait_send()

    for copy in raw:
        copy.wait_send()
    for z in range(2):
        part = rows.at[0, pl.ds(0, 3 * CAP)]
        remote(part, part, y_s.at[z], y_r.at[z, 0], other_z).wait_send()
        part = rows.at[pl.ds(0, 2)]
        remote(part, part, x_s.at[z], x_r.at[z, 0], other_z).wait_send()
    part = rows.at[pl.ds(0, 2)]
    remote(part, part, far_s.at[0], far_r.at[0], other_z).wait_send()
    for d in range(2):
        part = pair_recv.at[d]
        remote(part, part, pair_s.at[d], pair_r.at[d, 0], partner).wait_send()
    part = ret_recv.at[:, pl.ds(0, 15)]
    remote(part, part, ret_s.at[0], ret_r.at[0], other_z).wait_send()
    for d in range(2):
        place = 3 - zl if d == 0 else zl
        whole = hid.at[0]

        @pl.when(place < 3)
        def _():
            remote(line.at[d], line.at[d], line_s.at[d], line_r.at[d, 0], partner).wait_send()

        @pl.when(place > 0)
        def _():
            remote(whole, whole, cast_s.at[d], cast_r.at[d, 0], partner).wait_send()

        remote(whole, whole, core_s.at[d], core_r.at[d, 0], partner).wait_send()


def layer(tokens, out_grad, ids, probs, gate_weight, up_weight, down_weight):
    width, hid = gate_weight.shape
    tok = tokens.shape[0]
    total = CHUNKS * ROWS
    vm = pltpu.VMEM
    dma = pltpu.SemaphoreType.DMA
    inner = pl.BlockSpec(memory_space=pltpu.VMEM)
    outer = pl.BlockSpec(memory_space=pl.ANY)
    message = 3 * QUARTER
    return pl.pallas_call(
        functools.partial(kernel, width),
        out_shape=(
            vm((tok, width), BF16),
            vm((2, tok), F32),
            vm((width, hid), BF16),
            vm((width, hid), BF16),
            vm((hid, width), BF16),
        ),
        in_specs=[inner, inner, inner, inner, outer, outer, outer],
        out_specs=(inner,) * 5,
        scratch_shapes=[
            vm((2, tok, width), BF16),
            vm((2, tok), jnp.int32),
            vm((2, tok), BF16),
            vm((2, ROWS, tok), F32),
            vm((CHUNKS, ROWS, 2 * width + 128), BF16),
            vm((2, ROWS, 2 * width + 128), BF16),
            vm((4, width, 2 * QUARTER), BF16),
            vm((hid, width), BF16),
            vm((2, total, message), F32),
            vm((CHUNKS, 2, ROWS, message), F32),
            vm((2, total, message), F32),
            vm((2, total, message), BF16),
            vm((4, total, message), BF16),
            vm((CHUNKS, ROWS, width), BF16),
            vm((2, 16, CAP, width), BF16),
            vm((2, 16 * CAP, tok), BF16),
            vm((tok, width), BF16),
            vm((tok, width), BF16),
            vm((2, tok), F32),
            vm((2, tok), F32),
            vm((4, width, 2 * QUARTER), F32),
            vm((4, QUARTER, width), F32),
            vm((width, 2 * ROWS), BF16),
            vm((2 * ROWS, width), BF16),
            vm((NSUB, CAP, 128), BF16),
            vm((2, 16, CAP, 128), BF16),
            vm((8, 2, tok), F32),
            dma((2,)),
            dma((4,)),
            dma((4,)),
            dma((2,)),
            dma((2, 4)),
            dma((2,)),
            dma((2, 2)),
            dma((1,)),
            dma((2,)),
            dma((2,)),
            dma((2, CHUNKS + 3)),
            dma((2,)),
            dma((2, NSUB)),
            dma((2,)),
            dma((2, NSUB)),
            dma((2,)),
            dma((2, 2 * CHUNKS)),
            dma((1,)),
            dma((2,)),
            dma((2,)),
            dma((2,)),
            dma((1,)),
            dma((2,)),
            dma((1,)),
            dma((1,)),
        ],
        compiler_params=pltpu.CompilerParams(
            collective_id=0, has_side_effects=True, vmem_limit_bytes=55 * 1024 * 1024
        ),
    )(tokens, out_grad, ids, probs, gate_weight, up_weight, down_weight)


def spill(*refs):
    n = len(refs) // 2
    sems = refs[-1]
    copies = [pltpu.make_async_copy(refs[i], refs[n + i], sems.at[i]) for i in range(n)]
    for copy in copies:
        copy.start()
    for copy in copies:
        copy.wait()


def put(arrays):
    return pl.pallas_call(
        spill,
        out_shape=tuple(pltpu.HBM(a.shape, a.dtype) for a in arrays),
        in_specs=[pl.BlockSpec(memory_space=pltpu.VMEM)] * len(arrays),
        out_specs=(pl.BlockSpec(memory_space=pltpu.HBM),) * len(arrays),
        scratch_shapes=[pltpu.SemaphoreType.DMA((len(arrays),))],
        compiler_params=pltpu.CompilerParams(vmem_limit_bytes=16 * 1024 * 1024),
    )(*arrays)


def body(tokens, out_grad, expert_ids, gate_prob, gate_weight, up_weight, down_weight):
    input_grad, terms, gate_grad, up_grad, down_grad = put(
        layer(tokens, out_grad, expert_ids.T, gate_prob.T, gate_weight, up_weight, down_weight)
    )
    return (input_grad, terms.T, gate_grad, up_grad, down_grad)


def solution(mesh):
    return jax.shard_map(
        body,
        mesh=mesh,
        in_specs=(
            P("dp", "tensor"),
            P("dp", "tensor"),
            P("dp", None),
            P("dp", None),
            P("tensor", "dp"),
            P("tensor", "dp"),
            P("dp", "tensor"),
        ),
        out_specs=(
            P("dp", "tensor"),
            P("dp", None),
            P("tensor", "dp"),
            P("tensor", "dp"),
            P("dp", "tensor"),
        ),
        check_vma=False,
    )
```
